32 devices in a mesh: mem: 4 (over x, core), ty: 2 (over y), tx: 4 (over z).
Axes of the slice: x: 2, y: 2, z: 4, core: 2. Of those that a mesh axis runs over, the one named last changes fastest.
Arguments:
- pressure: float32 [8, 50, 64, 512], P('mem', None, 'ty', 'tx'), may hold values from -6 to 6
- east_wind: float32 [8, 50, 64, 512], P('mem', None, 'ty', 'tx'), may hold values from -6 to 6
- north_wind: float32 [8, 50, 64, 512], P('mem', None, 'ty', 'tx'), may hold values from -6 to 6
- vertical_wind: float32 [8, 49, 64, 512], P('mem', None, 'ty', 'tx'), may hold values from -6 to 6
- sound_squared: float32 [50, 64, 512], P(None, 'ty', 'tx'), may hold values from 0.5 to 2
- thickness: float32 [50], replicated, may hold values from 0.05 to 0.5
- owner_map: int32 [8], replicated, may hold values from 0 to 7, each once
Outputs:
- analysis: float32 [2, 4, 6, 32, 128], P('ty', 'tx', None, 'mem')
The draws below stay inside these ranges and needn't reach their ends.
Inputs may be any that keep to these rules, and one draw needn't show every extreme that they name: `owner_map`: every tile index appears exactly once.
All inputs are finite; a program needn't handle non-finite values.
Results may differ from the reference program's by a relative error of at most 0.0001.
Values sent between devices are 32-bit elements; how exact they have to be, the bound alone decides.
No kernel may reach another device: no remote copies, remote signals or barrier semaphores. Data moves between devices by JAX's collectives and lax.ppermute only.
A program may use at most 128 MiB of HBM per device.

```python
import math
import jax
import jax.numpy as jnp
from jax import lax

CY = 32
CX = 128
NZ = 50
SUBSTEPS = 2
MEMBERS = 8
NY = 64
NX = 512
WLEVELS = 49
TILES = 8
N_TY = 2
N_TX = 4


def levels(stream_key, dims, split, smallest, largest):
    def one(axis_at, parts):
        draws = jax.random.uniform(jax.random.fold_in(jax.random.fold_in(stream_key, 6), axis_at), (parts,), jnp.float32, smallest / len(split), largest / len(split))
        return jnp.repeat(jnp.exp(draws), dims[axis_at] // parts).reshape((-1,) + (1,) * (len(dims) - axis_at - 1))

    loudness = one(*split[0])
    for cut in split[1:]:
        loudness = loudness * one(*cut)
    return loudness


def noise(rng, shape, scale, most, pieces=(), held_as=jnp.bfloat16):
    array = jax.random.normal(rng, shape, jnp.float32) * scale
    if len(pieces) > 0:
        array = levels(rng, shape, pieces, -0.22, 0.18) * array
    return jnp.clip(array, min=-most, max=most).astype(held_as)


def setup_inputs(seed: int = 0) -> dict:
    key_list = jax.random.split(jax.random.key(seed), 8)
    return {
        "pressure": noise(key_list[0], (MEMBERS, NZ, NY, NX), 1.0, 6.0, ((0, 4), (2, 2), (3, 4)), jnp.float32),
        "east_wind": noise(key_list[1], (MEMBERS, NZ, NY, NX), 1.0, 6.0, ((0, 4), (2, 2), (3, 4)), jnp.float32),
        "north_wind": noise(key_list[2], (MEMBERS, NZ, NY, NX), 1.0, 6.0, ((0, 4), (2, 2), (3, 4)), jnp.float32),
        "vertical_wind": noise(key_list[3], (MEMBERS, WLEVELS, NY, NX), 1.0, 6.0, ((0, 4), (2, 2), (3, 4)), jnp.float32),
        "sound_squared": jnp.clip(jnp.exp(math.log(2.0) - 1.3862944 * jax.random.uniform(key_list[4], (NZ, NY, NX), jnp.float32) ** levels(key_list[4], (NZ, NY, NX), ((1, 2), (2, 4)), -0.2, 0.2)), 0.5, 2.0),
        "thickness": jnp.clip(jnp.exp(jax.random.uniform(key_list[5], (NZ,), jnp.float32, math.log(0.05), math.log(0.5))), 0.05, 0.5),
        "owner_map": jax.random.permutation(key_list[6], TILES).astype(jnp.int32),
    }


horiz_ratio = 0.35
vert_ratio = 1.5


def column_solve(coeff, rhs_list):
    count = len(rhs_list)
    factors = []
    values = []
    pivot = 1.0 + coeff[1] + coeff[0]
    values.append(rhs_list[0] / pivot)
    factors.append(-coeff[1] / pivot)
    for position in range(1, count):
        pivot = (1.0 + coeff[position + 1] + coeff[position]) + coeff[position] * factors[position - 1]
        values.append((rhs_list[position] + coeff[position] * values[position - 1]) / pivot)
        factors.append(-coeff[position + 1] / pivot)
    solved = [values[count - 1]]
    for position in range(count - 2, -1, -1):
        solved.insert(0, values[position] - factors[position] * solved[0])
    return solved


def member_run(pressure, east_wind, north_wind, vertical_wind, sound_squared, thickness):
    coeff_field = vert_ratio * vert_ratio * sound_squared
    coeff = [coeff_field[level] for level in range(NZ)]
    for substep in range(SUBSTEPS):
        east_wind = east_wind - horiz_ratio * (pressure - jnp.roll(pressure, 1, axis=2))
        north_wind = north_wind - horiz_ratio * (pressure - jnp.roll(pressure, 1, axis=1))
        divergence = (jnp.roll(east_wind, -1, axis=2) - east_wind) + (jnp.roll(north_wind, -1, axis=1) - north_wind)
        partial_value = pressure - horiz_ratio * sound_squared * divergence
        rhs_list = [vertical_wind[level] - vert_ratio * (partial_value[level + 1] - partial_value[level]) for level in range(NZ - 1)]
        vertical_wind = jnp.stack(column_solve(coeff, rhs_list), axis=0)
        zero_layer = jnp.zeros_like(partial_value[:1])
        padded = jnp.concatenate([zero_layer, vertical_wind, zero_layer], axis=0)
        pressure = partial_value - vert_ratio * sound_squared * (padded[1:] - padded[:-1])
    mass = jnp.einsum('k,kyx->yx', thickness, pressure, precision=lax.Precision.HIGHEST)
    east_total = jnp.einsum('k,kyx->yx', thickness, east_wind, precision=lax.Precision.HIGHEST)
    north_total = jnp.einsum('k,kyx->yx', thickness, north_wind, precision=lax.Precision.HIGHEST)
    return jnp.stack([mass, east_total, north_total], axis=0)


def reference(pressure, east_wind, north_wind, vertical_wind, sound_squared, thickness, owner_map):
    def one_member(fields):
        return member_run(fields[0], fields[1], fields[2], fields[3], sound_squared, thickness)

    integrals = lax.map(one_member, (pressure, east_wind, north_wind, vertical_wind))
    mean = jnp.sum(integrals, axis=0) / MEMBERS
    variance = jnp.sum((integrals - mean) ** 2, axis=0) / (MEMBERS - 1)
    stats = jnp.concatenate([mean, variance], axis=0)
    tiled = stats.reshape(6, N_TY, CY, N_TX, CX).transpose(1, 3, 0, 2, 4).reshape(N_TY * N_TX, 6, CY, CX)
    placed = jnp.zeros_like(tiled).at[owner_map.astype(jnp.int32)].set(tiled)
    return placed.reshape(N_TY, N_TX, 6, CY, CX)
```

```python
import functools

import jax
import jax.numpy as jnp
from jax import lax
from jax.experimental import pallas as pl
from jax.experimental.pallas import tpu as pltpu
from jax.sharding import PartitionSpec as P

HORIZ = 0.35
VERT = 1.5

VMEM = pl.BlockSpec(memory_space=pltpu.VMEM)
SMEM = pl.BlockSpec(memory_space=pltpu.SMEM)


def divisor(count, most):
    return max(d for d in range(1, most + 1) if count % d == 0)


def lanes_of(shape):
    return lax.broadcasted_iota(jnp.int32, shape, len(shape) - 1)


def rows_of(shape):
    return lax.broadcasted_iota(jnp.int32, shape, len(shape) - 2)


def west_roll(x):
    return pltpu.roll(x, 1, 1)


def east_roll(x):
    return pltpu.roll(x, x.shape[1] - 1, 1)


def south_roll(x):
    return pltpu.roll(x, 1, 0)


def north_roll(x):
    return pltpu.roll(x, x.shape[0] - 1, 0)


def pack_kernel(p_ref, u_ref, v_ref, cols_ref, rows_ref):
    members, levels, rows, cols = p_ref.shape
    lane = lanes_of((rows, cols))
    for m in range(members):
        packed = jnp.zeros((rows, cols), jnp.float32)
        for k in range(levels):
            p = p_ref[m, k]
            z = u_ref[m, k] - HORIZ * p
            edge = pltpu.roll(jnp.where(lane == cols - 1, p, z), 2 * k + 1, 1)
            packed = jnp.where(lane >= 2 * k, edge, packed)
            rows_ref[0, m, k : k + 1, :] = p[rows - 1 : rows, :]
            rows_ref[1, m, k : k + 1, :] = v_ref[m, k, 0:1, :] - HORIZ * p[0:1, :]
        cols_ref[m] = packed


def main_kernel(
    p_ref, u_ref, v_ref, w_ref, c_ref, th_ref, from_west, from_east, from_rows,
    sums_ref, cols_ref, rows_ref, hcols_ref, hrows_ref,
    e_s, inv_s, s_s, g_s, h_s, hw_s, he_s, hs_s, hn_s, part_s, v_s, u1_s, v1_s,
):
    members, levels, rows, cols = p_ref.shape
    inner = levels - 1
    shape = (rows, cols)
    lane = lanes_of(shape)
    row = rows_of(shape)
    first_lane, last_lane = lane == 0, lane == cols - 1
    first_row, last_row = row == 0, row == rows - 1
    zero = jnp.zeros(shape, jnp.float32)
    vsq = VERT * VERT

    step = divisor(inner, 8)

    def factor(chunk, carry):
        e_prev, s_prev, c_here = carry
        for sub in range(step):
            i = chunk * step + sub
            c_next = c_ref[i + 1]
            b_next = vsq * c_next
            pivot = (1.0 + b_next) + (vsq * c_here) * (1.0 - e_prev)
            inv = 1.0 / pivot
            s_prev = VERT * (th_ref[i + 1] * c_next - th_ref[i] * c_here) + e_prev * s_prev
            e_prev = b_next * inv
            e_s[i] = e_prev
            inv_s[i] = inv
            s_s[i] = s_prev * inv
            c_here = c_next
        return e_prev, s_prev, c_here

    lax.fori_loop(0, inner // step, factor, (zero, zero, c_ref[0]))

    def weights(k, y_above, y_here):
        g = th_ref[k] + VERT * (y_above - y_here)
        h = g * (HORIZ * c_ref[k])
        g_s[k] = g - (2 * HORIZ) * h
        h_s[k] = h
        h35 = HORIZ * h
        hw_s[k] = jnp.where(first_lane, 0.0, west_roll(h))
        he_s[k] = jnp.where(last_lane, 0.0, east_roll(h35))
        hs_s[k] = jnp.where(first_row, 0.0, south_roll(h))
        hn_s[k] = jnp.where(last_row, 0.0, north_roll(h35))
        hrows_ref[0, pl.ds(k, 1), :] = h35[0:1, :]
        hrows_ref[1, pl.ds(k, 1), :] = h[rows - 1 : rows, :]
        return west_roll(jnp.where(last_lane, -h, h35))

    def adjoint(chunk, carry):
        y_above, packed = carry
        for sub in range(step):
            i = inner - 1 - (chunk * step + sub)
            y_here = s_s[i] + e_s[i] * y_above
            s_s[i] = y_here
            edge = weights(i + 1, y_above, y_here)
            packed = jnp.where(lane < 2, edge, pltpu.roll(packed, 2, 1))
            y_above = y_here
        return y_above, packed

    y_low, packed = lax.fori_loop(0, inner // step, adjoint, (zero, zero))
    edge = weights(0, y_low, zero)
    hcols_ref[...] = jnp.where(lane < 2, edge, pltpu.roll(packed, 2, 1))

    step1 = divisor(levels, 5)
    halo = []
    even = lane % 2 == 0
    for m in range(members):
        mixed = jnp.where(even, east_roll(from_east[m]), HORIZ * west_roll(from_west[m]))
        halo.append(east_roll(mixed))

    def upward(chunk, carry):
        part_prev, v_prev, halo = (list(x) for x in carry)
        for sub in range(step1):
            k = chunk * step1 + sub
            c = c_ref[k]
            c35 = HORIZ * c
            below = jnp.maximum(k - 1, 0)
            before = jnp.maximum(k - 2, 0)
            e = e_s[before]
            for m in range(members):
                p = p_ref[m, k]
                q = HORIZ * p
                zu = u_ref[m, k] - q
                zv = v_ref[m, k] - q
                edge = halo[m] if sub == 0 else pltpu.roll(halo[m], cols - 2 * sub, 1)
                q_west = jnp.where(first_lane, edge, west_roll(q))
                zu_east = jnp.where(last_lane, edge, east_roll(zu))
                q_south = jnp.where(first_row, HORIZ * from_rows[0, m, pl.ds(k, 1), :], south_roll(q))
                zv_north = jnp.where(last_row, from_rows[1, m, pl.ds(k, 1), :], north_roll(zv))
                u1 = zu + q_west
                v1 = zv + q_south
                u1_s[m, k] = u1
                v1_s[m, k] = v1
                div = ((zu_east + q) - u1) + ((zv_north + q) - v1)
                part = p - c35 * div
                part_s[m, k] = part
                rhs = w_ref[m, below] - VERT * (part - part_prev[m])
                v_new = rhs + e * v_prev[m]
                v_s[m, below] = v_new
                if sub == 0:
                    v_new = jnp.where(k == 0, 0.0, v_new)
                v_prev[m] = v_new
                part_prev[m] = part
        halo = [pltpu.roll(x, cols - 2 * step1, 1) for x in halo]
        return tuple(part_prev), tuple(v_prev), tuple(halo)

    zeros = (zero,) * members
    lax.fori_loop(0, levels // step1, upward, (zeros, zeros, tuple(halo)))

    group = 8
    gshape = (group, cols)
    glane = lanes_of(gshape)
    glast = glane == cols - 1
    gzero = jnp.zeros(gshape, jnp.float32)
    for r in range(rows // group):
        rs = slice(r * group, (r + 1) * group)

        def downward(chunk, carry, r=r, rs=rs):
            state = [list(x) for x in carry]
            for sub in range(step1):
                k = levels - 1 - (chunk * step1 + sub)
                below = jnp.maximum(k - 1, 0)
                inv = inv_s[below, rs]
                e = e_s[below, rs]
                c15 = VERT * c_ref[k, rs]
                g = g_s[k, rs]
                y = s_s[below, rs]
                h = h_s[k, rs]
                hw, he, hs, hn = hw_s[k, rs], he_s[k, rs], hs_s[k, rs], hn_s[k, rs]
                th = th_ref[k]
                for m in range(members):
                    w, mass, ps, us, vs, ce, cw, cn, cs, packed = state[m]
                    w_low = v_s[m, below, rs] * inv + e * w
                    if sub == step1 - 1:
                        w_low = jnp.where(k == 0, 0.0, w_low)
                    p = part_s[m, k, rs] - c15 * (w - w_low)
                    q = HORIZ * p
                    zu = u1_s[m, k, rs] - q
                    zv = v1_s[m, k, rs] - q
                    mass = mass + ((g * p + y * w_low) + h * (zu + zv))
                    ps = ps + th * p
                    us = us + th * zu
                    vs = vs + th * zv
                    ce = ce + hw * zu
                    cw = cw + he * p
                    cn = cn + hs * zv
                    cs = cs + hn * p
                    edge = pltpu.roll(jnp.where(glast, p, zu), 1, 1)
                    packed = jnp.where(glane < 2, edge, pltpu.roll(packed, 2, 1))
                    if r == rows // group - 1:
                        rows_ref[0, m, pl.ds(k, 1), :] = p[group - 1 : group, :]
                    if r == 0:
                        rows_ref[1, m, pl.ds(k, 1), :] = zv[0:1, :]
                    state[m] = [w_low, mass, ps, us, vs, ce, cw, cn, cs, packed]
            return tuple(tuple(x) for x in state)

        init = ((gzero,) * 10,) * members
        out = lax.fori_loop(0, levels // step1, downward, init)
        for m in range(members):
            w, mass, ps, us, vs, ce, cw, cn, cs, packed = out[m]
            sums_ref[m, 0, rs] = mass - east_roll(ce) + west_roll(cw)
            sums_ref[m, 1, rs] = us + jnp.where(glane == 0, 0.0, HORIZ * west_roll(ps))
            sums_ref[m, 2, rs] = vs
            tail = pltpu.roll(ps, 2 * levels + 1, 1)
            cols_ref[m, rs] = jnp.where(glane == 2 * levels, tail, packed)
            part_s[m, 0, rs] = ps
            part_s[m, 1, rs] = cn
            part_s[m, 2, rs] = cs
    for m in range(members):
        ps, cn, cs = part_s[m, 0], part_s[m, 1], part_s[m, 2]
        sums_ref[m, 0] = sums_ref[m, 0] - north_roll(cn) + south_roll(cs)
        sums_ref[m, 2] = sums_ref[m, 2] + jnp.where(first_row, 0.0, HORIZ * south_roll(ps))
        rows_ref[0, m, levels : levels + 1, :] = ps[rows - 1 : rows, :]
        rows_ref[1, m, levels : levels + 1, :] = jnp.zeros((1, cols), jnp.float32)


def edge_kernel(sums_ref, from_west, from_east, from_rows, hcols_ref, hrows_ref, out_ref):
    members, fields, rows, cols = sums_ref.shape
    levels = hrows_ref.shape[1]
    quarters = out_ref.shape[0]
    height = rows // quarters
    lane = lanes_of((rows, cols))
    row = rows_of((rows, cols))
    even = lane % 2 == 0
    used = lane < 2 * levels
    for m in range(members):
        west = from_west[m]
        east = east_roll(from_east[m])
        products = jnp.where(used, hcols_ref[...] * jnp.where(even, east, west_roll(west)), 0.0)
        at_east = jnp.sum(jnp.where(even, products, 0.0), axis=1, keepdims=True)
        at_west = jnp.sum(jnp.where(even, 0.0, products), axis=1, keepdims=True)
        at_south = jnp.sum(hrows_ref[0] * from_rows[0, m, :levels, :], axis=0, keepdims=True)
        at_north = jnp.sum(hrows_ref[1] * from_rows[1, m, :levels, :], axis=0, keepdims=True)
        ps_west = pltpu.roll(west, cols - 2 * levels, 1)
        ps_south = from_rows[0, m, levels : levels + 1, :]
        mass = sums_ref[m, 0] + jnp.where(lane == 0, at_west, 0.0) + jnp.where(lane == cols - 1, at_east, 0.0)
        mass = mass + jnp.where(row == 0, at_south, 0.0) - jnp.where(row == rows - 1, at_north, 0.0)
        east_total = sums_ref[m, 1] + jnp.where(lane == 0, HORIZ * ps_west, 0.0)
        north_total = sums_ref[m, 2] + jnp.where(row == 0, HORIZ * ps_south, 0.0)
        for f, total in enumerate((mass, east_total, north_total)):
            for q in range(quarters):
                out_ref[q, m, f] = total[q * height : (q + 1) * height, :]


def stats_kernel(in_ref, out_ref):
    ranks, members, fields, height, cols = in_ref.shape
    slots = out_ref.shape[0]
    count = ranks * members
    for f in range(fields):
        values = [in_ref[r, m, f] for r in range(ranks) for m in range(members)]
        mean = functools.reduce(jnp.add, values) / count
        square = functools.reduce(jnp.add, [(v - mean) * (v - mean) for v in values]) / (count - 1)
        for s in range(slots):
            out_ref[s, f] = mean
            out_ref[s, fields + f] = square


def pick_kernel(owner_ref, me_ref, in_ref, out_ref):
    me = me_ref[0]
    source = jnp.int32(0)
    for t in range(in_ref.shape[0]):
        source = jnp.where(owner_ref[t] == me, t, source)
    out_ref[0, 0] = in_ref[source]


def call(kernel, outs, in_specs, scratch=(), limit=None):
    return pl.pallas_call(
        kernel,
        out_shape=[jax.ShapeDtypeStruct(s, jnp.float32) for s in outs],
        in_specs=in_specs,
        out_specs=[VMEM] * len(outs),
        scratch_shapes=list(scratch),
        compiler_params=pltpu.CompilerParams(vmem_limit_bytes=limit),
    )


def shifted(block, axis, distance):
    count = lax.axis_size(axis)
    return lax.ppermute(block, axis, [((i - distance) % count, i) for i in range(count)])


def exchange(columns, edge_rows):
    west = shifted(columns, "tx", 1)
    east = shifted(columns, "tx", -1)
    if lax.axis_size("ty") <= 2:
        both = shifted(edge_rows, "ty", 1)
    else:
        south = shifted(edge_rows[0], "ty", 1)
        north = shifted(edge_rows[1], "ty", -1)
        both = jnp.stack([south, north])
    return west, east, both


def local(pressure, east_wind, north_wind, vertical_wind, sound_squared, thickness, owner_map):
    members, levels, rows, cols = pressure.shape
    ranks = lax.axis_size("mem")
    tiles = lax.axis_size("ty") * lax.axis_size("tx")
    height = rows // ranks
    mib = 1024 * 1024
    plane = (members, rows, cols)
    columns, edge_rows = call(
        pack_kernel, [plane, (2, members, levels + 1, cols)], [VMEM] * 3, limit=16 * mib
    )(pressure, east_wind, north_wind)
    west, east, both = exchange(columns, edge_rows)
    field = pltpu.VMEM((levels, rows, cols), jnp.float32)
    many = pltpu.VMEM((members, levels, rows, cols), jnp.float32)
    sums, columns, edge_rows, hcols, hrows = call(
        main_kernel,
        [
            (members, 3, rows, cols),
            plane,
            (2, members, levels + 1, cols),
            (rows, cols),
            (2, levels, cols),
        ],
        [VMEM] * 5 + [SMEM] + [VMEM] * 3,
        [field] * 9 + [many] * 4,
        limit=32 * mib,
    )(
        pressure, east_wind, north_wind, vertical_wind, sound_squared, thickness, west, east, both
    )
    west, east, both = exchange(columns, edge_rows)
    (integrals,) = call(
        edge_kernel, [(ranks, members, 3, height, cols)], [VMEM] * 6, limit=16 * mib
    )(sums, west, east, both, hcols, hrows)
    gathered = lax.all_to_all(integrals, "mem", 0, 0)
    (slots,) = call(stats_kernel, [(tiles, 6, height, cols)], [VMEM], limit=16 * mib)(gathered)
    routed = lax.all_to_all(slots, ("ty", "tx"), 0, 0)
    me = lax.axis_index(("ty", "tx")).astype(jnp.int32).reshape(1)
    (result,) = call(
        pick_kernel, [(1, 1, 6, height, cols)], [SMEM, SMEM, VMEM], limit=16 * mib
    )(owner_map, me, routed)
    return result


def solution(mesh):
    placed = (
        P("mem", None, "ty", "tx"),
        P("mem", None, "ty", "tx"),
        P("mem", None, "ty", "tx"),
        P("mem", None, "ty", "tx"),
        P(None, "ty", "tx"),
        P(),
        P(),
    )
    return jax.shard_map(
        local,
        mesh=mesh,
        in_specs=placed,
        out_specs=P("ty", "tx", None, "mem", None),
        check_vma=False,
    )
```

```python
import functools

import jax
import jax.numpy as jnp
from jax import lax
from jax.experimental import pallas as pl
from jax.experimental.pallas import tpu as pltpu
from jax.sharding import PartitionSpec as P

HORIZ = 0.35
VERT = 1.5
STEP_A = 50
STEP_B = 25

VMEM = pl.BlockSpec(memory_space=pltpu.VMEM)
SMEM = pl.BlockSpec(memory_space=pltpu.SMEM)
HBM = pl.BlockSpec(memory_space=pltpu.HBM)


def divisor(count, most):
    return max(d for d in range(1, most + 1) if count % d == 0)


def lanes_of(shape):
    return lax.broadcasted_iota(jnp.int32, shape, len(shape) - 1)


def rows_of(shape):
    return lax.broadcasted_iota(jnp.int32, shape, len(shape) - 2)


def west_roll(x):
    return pltpu.roll(x, 1, 1)


def east_roll(x):
    return pltpu.roll(x, x.shape[1] - 1, 1)


def south_roll(x):
    return pltpu.roll(x, 1, 0)


def north_roll(x):
    return pltpu.roll(x, x.shape[0] - 1, 0)


def pack_kernel(p_hbm, u_hbm, v_hbm, cols_ref, rows_ref, p_ref, u_ref, v_s, sems):
    members, levels, rows, cols = p_ref.shape
    copies = []
    for m in range(members):
        pair = [
            pltpu.make_async_copy(p_hbm.at[m], p_ref.at[m], sems.at[m, 0]),
            pltpu.make_async_copy(u_hbm.at[m], u_ref.at[m], sems.at[m, 1]),
            pltpu.make_async_copy(v_hbm.at[m, :, 0:8], v_s.at[m], sems.at[m, 2]),
        ]
        for copy in pair:
            copy.start()
        copies.append(pair)
    lane = lanes_of((rows, cols))
    for m in range(members):
        for copy in copies[m]:
            copy.wait()
        packed = jnp.zeros((rows, cols), jnp.float32)
        for k in range(levels):
            p = p_ref[m, k]
            z = u_ref[m, k] - HORIZ * p
            edge = pltpu.roll(jnp.where(lane == cols - 1, p, z), 2 * k + 1, 1)
            packed = jnp.where(lane >= 2 * k, edge, packed)
            rows_ref[0, m, k : k + 1, :] = p[rows - 1 : rows, :]
            rows_ref[1, m, k : k + 1, :] = v_s[m, k, 0:1, :] - HORIZ * p[0:1, :]
        rows_ref[0, m, levels : levels + 1, :] = jnp.zeros((1, cols), jnp.float32)
        rows_ref[1, m, levels : levels + 1, :] = jnp.zeros((1, cols), jnp.float32)
        cols_ref[m] = packed


def weight_kernel(
    c_ref, v_hbm, w_hbm, th_ref,
    hcols_ref, hrows_ref, e_s, inv_s, s_s, g_s, h_s, hw_s, he_s, hs_s, hn_s, v_ref, w_ref, sems,
):
    levels, rows, cols = c_ref.shape
    copies = [
        pltpu.make_async_copy(v_hbm, v_ref, sems.at[0]),
        pltpu.make_async_copy(w_hbm, w_ref, sems.at[1]),
    ]
    for copy in copies:
        copy.start()
    inner = levels - 1
    shape = (rows, cols)
    lane = lanes_of(shape)
    row = rows_of(shape)
    first_lane, last_lane = lane == 0, lane == cols - 1
    first_row, last_row = row == 0, row == rows - 1
    zero = jnp.zeros(shape, jnp.float32)
    vsq = VERT * VERT

    step = divisor(inner, STEP_A)

    def factor(chunk, carry):
        e_prev, s_prev, c_here = carry
        for sub in range(step):
            i = chunk * step + sub
            c_next = c_ref[i + 1]
            b_next = vsq * c_next
            pivot = (1.0 + b_next) + (vsq * c_here) * (1.0 - e_prev)
            inv = 1.0 / pivot
            s_prev = VERT * (th_ref[i + 1] * c_next - th_ref[i] * c_here) + e_prev * s_prev
            e_prev = b_next * inv
            e_s[i] = e_prev
            inv_s[i] = inv
            s_s[i] = s_prev * inv
            c_here = c_next
        return e_prev, s_prev, c_here

    lax.fori_loop(0, inner // step, factor, (zero, zero, c_ref[0]))

    def weights(k, y_above, y_here):
        g = th_ref[k] + VERT * (y_above - y_here)
        h = g * (HORIZ * c_ref[k])
        g_s[k] = g - (2 * HORIZ) * h
        h_s[k] = h
        h35 = HORIZ * h
        hw_s[k] = jnp.where(first_lane, 0.0, west_roll(h))
        he_s[k] = jnp.where(last_lane, 0.0, east_roll(h35))
        hs_s[k] = jnp.where(first_row, 0.0, south_roll(h))
        hn_s[k] = jnp.where(last_row, 0.0, north_roll(h35))
        hrows_ref[0, pl.ds(k, 1), :] = h35[0:1, :]
        hrows_ref[1, pl.ds(k, 1), :] = h[rows - 1 : rows, :]
        return jnp.where(last_lane, -h, h35)

    def adjoint(chunk, carry):
        y_above, packed = carry
        packed = pltpu.roll(packed, 2 * step, 1)
        for sub in range(step):
            i = inner - 1 - (chunk * step + sub)
            y_here = s_s[i] + e_s[i] * y_above
            s_s[i] = y_here
            edge = weights(i + 1, y_above, y_here)
            place = 2 * (step - 1 - sub)
            packed = jnp.where(lane < place + 2, pltpu.roll(edge, place + 1, 1), packed)
            y_above = y_here
        return y_above, packed

    y_low, packed = lax.fori_loop(0, inner // step, adjoint, (zero, zero))
    edge = weights(0, y_low, zero)
    hcols_ref[...] = jnp.where(lane < 2, pltpu.roll(edge, 1, 1), pltpu.roll(packed, 2, 1))
    for copy in copies:
        copy.wait()


def main_kernel(
    p_ref, u_ref, v_ref, w_ref, c_ref, th_ref, e_s, inv_s, s_s, g_s, h_s, hw_s, he_s, hs_s, hn_s,
    from_west, from_east, from_rows,
    sums_ref, cols_ref, rows_ref,
    part_s, v_s, u1_s, v1_s,
):
    members, levels, rows, cols = p_ref.shape
    shape = (rows, cols)
    lane = lanes_of(shape)
    row = rows_of(shape)
    first_lane, last_lane = lane == 0, lane == cols - 1
    first_row, last_row = row == 0, row == rows - 1
    zero = jnp.zeros(shape, jnp.float32)

    step1 = divisor(levels, STEP_B)
    halo = []
    even = lane % 2 == 0
    for m in range(members):
        mixed = jnp.where(even, east_roll(from_east[m]), HORIZ * west_roll(from_west[m]))
        halo.append(east_roll(mixed))

    def upward(chunk, carry):
        part_prev, v_prev, halo = (list(x) for x in carry)
        for sub in range(step1):
            k = chunk * step1 + sub
            c = c_ref[k]
            c35 = HORIZ * c
            below = jnp.maximum(k - 1, 0)
            before = jnp.maximum(k - 2, 0)
            e = e_s[before]
            for m in range(members):
                p = p_ref[m, k]
                q = HORIZ * p
                zu = u_ref[m, k] - q
                zv = v_ref[m, k] - q
                edge = halo[m] if sub == 0 else pltpu.roll(halo[m], cols - 2 * sub, 1)
                q_west = jnp.where(first_lane, edge, west_roll(q))
                zu_east = jnp.where(last_lane, edge, east_roll(zu))
                q_south = jnp.where(first_row, HORIZ * from_rows[0, m, pl.ds(k, 1), :], south_roll(q))
                zv_north = jnp.where(last_row, from_rows[1, m, pl.ds(k, 1), :], north_roll(zv))
                u1 = zu + q_west
                v1 = zv + q_south
                u1_s[m, k] = u1
                v1_s[m, k] = v1
                div = ((zu_east + q) - u1) + ((zv_north + q) - v1)
                part = p - c35 * div
                part_s[m, k] = part
                rhs = w_ref[m, below] - VERT * (part - part_prev[m])
                v_new = rhs + e * v_prev[m]
                v_s[m, below] = v_new
                if sub == 0:
                    v_new = jnp.where(k == 0, 0.0, v_new)
                v_prev[m] = v_new
                part_prev[m] = part
        halo = [pltpu.roll(x, cols - 2 * step1, 1) for x in halo]
        return tuple(part_prev), tuple(v_prev), tuple(halo)

    zeros = (zero,) * members
    lax.fori_loop(0, levels // step1, upward, (zeros, zeros, tuple(halo)))

    group = 8
    gshape = (group, cols)
    glane = lanes_of(gshape)
    glast = glane == cols - 1
    gzero = jnp.zeros(gshape, jnp.float32)
    for r in range(rows // group):
        rs = slice(r * group, (r + 1) * group)

        def downward(chunk, carry, r=r, rs=rs):
            state = [list(x) for x in carry]
            for sub in range(step1):
                k = levels - 1 - (chunk * step1 + sub)
                below = jnp.maximum(k - 1, 0)
                inv = inv_s[below, rs]
                e = e_s[below, rs]
                c15 = VERT * c_ref[k, rs]
                g = g_s[k, rs]
                y = s_s[below, rs]
                h = h_s[k, rs]
                hw, he, hs, hn = hw_s[k, rs], he_s[k, rs], hs_s[k, rs], hn_s[k, rs]
                th = th_ref[k]
                for m in range(members):
                    w, mass, ps, us, vs, ce, cw, cn, cs, packed = state[m]
                    w_low = v_s[m, below, rs] * inv + e * w
                    if sub == step1 - 1:
                        w_low = jnp.where(k == 0, 0.0, w_low)
                    p = part_s[m, k, rs] - c15 * (w - w_low)
                    q = HORIZ * p
                    zu = u1_s[m, k, rs] - q
                    zv = v1_s[m, k, rs] - q
                    mass = mass + ((g * p + y * w_low) + h * (zu + zv))
                    ps = ps + th * p
                    us = us + th * zu
                    vs = vs + th * zv
                    ce = ce + hw * zu
                    cw = cw + he * p
                    cn = cn + hs * zv
                    cs = cs + hn * p
                    place = 2 * (step1 - 1 - sub)
                    edge = pltpu.roll(jnp.where(glast, p, zu), place + 1, 1)
                    if sub == 0:
                        packed = pltpu.roll(packed, 2 * step1, 1)
                    packed = jnp.where(glane < place + 2, edge, packed)
                    if r == rows // group - 1:
                        rows_ref[0, m, pl.ds(k, 1), :] = p[group - 1 : group, :]
                    if r == 0:
                        rows_ref[1, m, pl.ds(k, 1), :] = zv[0:1, :]
                    state[m] = [w_low, mass, ps, us, vs, ce, cw, cn, cs, packed]
            return tuple(tuple(x) for x in state)

        init = ((gzero,) * 10,) * members
        out = lax.fori_loop(0, levels // step1, downward, init)
        for m in range(members):
            w, mass, ps, us, vs, ce, cw, cn, cs, packed = out[m]
            sums_ref[m, 0, rs] = mass - east_roll(ce) + west_roll(cw)
            sums_ref[m, 1, rs] = us + jnp.where(glane == 0, 0.0, HORIZ * west_roll(ps))
            sums_ref[m, 2, rs] = vs
            tail = pltpu.roll(ps, 2 * levels + 1, 1)
            cols_ref[m, rs] = jnp.where(glane == 2 * levels, tail, packed)
            part_s[m, 0, rs] = ps
            part_s[m, 1, rs] = cn
            part_s[m, 2, rs] = cs
    for m in range(members):
        ps, cn, cs = part_s[m, 0], part_s[m, 1], part_s[m, 2]
        sums_ref[m, 0] = sums_ref[m, 0] - north_roll(cn) + south_roll(cs)
        sums_ref[m, 2] = sums_ref[m, 2] + jnp.where(first_row, 0.0, HORIZ * south_roll(ps))
        rows_ref[0, m, levels : levels + 1, :] = ps[rows - 1 : rows, :]
        rows_ref[1, m, levels : levels + 1, :] = jnp.zeros((1, cols), jnp.float32)


def edge_kernel(sums_ref, from_west, from_east, from_rows, hcols_ref, hrows_ref, *rest):
    outs, total_s = rest[:-1], rest[-1]
    members, fields, rows, cols = sums_ref.shape
    levels = hrows_ref.shape[1]
    height = rows // len(outs)
    mine = lax.axis_index("mem")
    lane = lanes_of((rows, cols))
    row = rows_of((rows, cols))
    even = lane % 2 == 0
    used = lane < 2 * levels
    for m in range(members):
        west = from_west[m]
        east = east_roll(from_east[m])
        products = jnp.where(used, hcols_ref[...] * jnp.where(even, east, west_roll(west)), 0.0)
        at_east = jnp.sum(jnp.where(even, products, 0.0), axis=1, keepdims=True)
        at_west = jnp.sum(jnp.where(even, 0.0, products), axis=1, keepdims=True)
        at_south = jnp.sum(hrows_ref[0] * from_rows[0, m, :levels, :], axis=0, keepdims=True)
        at_north = jnp.sum(hrows_ref[1] * from_rows[1, m, :levels, :], axis=0, keepdims=True)
        ps_west = pltpu.roll(west, cols - 2 * levels, 1)
        ps_south = from_rows[0, m, levels : levels + 1, :]
        mass = sums_ref[m, 0] + jnp.where(lane == 0, at_west, 0.0) + jnp.where(lane == cols - 1, at_east, 0.0)
        mass = mass + jnp.where(row == 0, at_south, 0.0) - jnp.where(row == rows - 1, at_north, 0.0)
        total_s[m, 0] = mass
        total_s[m, 1] = sums_ref[m, 1] + jnp.where(lane == 0, HORIZ * ps_west, 0.0)
        total_s[m, 2] = sums_ref[m, 2] + jnp.where(row == 0, HORIZ * ps_south, 0.0)
    for d, out_ref in enumerate(outs):
        start = pl.multiple_of((mine ^ d) * height, height)
        out_ref[...] = total_s[:, :, pl.ds(start, height), :]


def stats_kernel(*refs):
    ins, out_ref = refs[:-1], refs[-1]
    members, fields = ins[0].shape[:2]
    count = len(ins) * members
    for f in range(fields):
        values = [ref[m, f] for ref in ins for m in range(members)]
        mean = functools.reduce(jnp.add, values) / count
        square = functools.reduce(jnp.add, [(v - mean) * (v - mean) for v in values]) / (count - 1)
        out_ref[f] = mean
        out_ref[fields + f] = square


def select_kernel(width, owner_ref, *refs):
    tiles, outs = refs[: -width], refs[-width :]
    row, column = lax.axis_index("ty"), lax.axis_index("tx")
    for d, out_ref in enumerate(outs):
        target = row * width + (column ^ d)
        value = tiles[0][...]
        for j in range(1, len(tiles)):
            here = owner_ref[(row ^ j) * width + column] == target
            value = jnp.where(here, tiles[j][...], value)
        out_ref[...] = value


def pick_kernel(height_count, owner_ref, *refs):
    ins, out_ref = refs[:-1], refs[-1]
    width = len(ins)
    row, column = lax.axis_index("ty"), lax.axis_index("tx")
    me = row * width + column
    value = ins[0][...]
    for d in range(1, width):
        source = column ^ d
        here = owner_ref[source] == me
        for j in range(1, height_count):
            here = here | (owner_ref[j * width + source] == me)
        value = jnp.where(here, ins[d][...], value)
    out_ref[0, 0] = value


def call(kernel, outs, in_specs, scratch=(), limit=16):
    return pl.pallas_call(
        kernel,
        out_shape=[jax.ShapeDtypeStruct(s, jnp.float32) for s in outs],
        in_specs=in_specs,
        out_specs=[VMEM] * len(outs),
        scratch_shapes=list(scratch),
        compiler_params=pltpu.CompilerParams(vmem_limit_bytes=limit * 1024 * 1024),
    )


def permuted(block, axis, source):
    count = lax.axis_size(axis)
    return lax.ppermute(block, axis, [(source(i) % count, i) for i in range(count)])


def exchange(columns, edge_rows):
    if lax.axis_size("ty") <= 2:
        both = permuted(edge_rows, "ty", lambda i: i - 1)
    else:
        south = permuted(edge_rows[0], "ty", lambda i: i - 1)
        north = permuted(edge_rows[1], "ty", lambda i: i + 1)
        both = jnp.stack([south, north])
    west = permuted(columns, "tx", lambda i: i - 1)
    east = permuted(columns, "tx", lambda i: i + 1)
    return west, east, both


def local(pressure, east_wind, north_wind, vertical_wind, sound_squared, thickness, owner_map):
    members, levels, rows, cols = pressure.shape
    ranks, height_count, width = (lax.axis_size(a) for a in ("mem", "ty", "tx"))
    height = rows // ranks
    plane = (members, rows, cols)
    many = (members, levels, rows, cols)
    field = (levels, rows, cols)
    lines = (2, members, levels + 1, cols)
    part = (6, height, cols)
    columns, edge_rows = call(
        pack_kernel,
        [plane, lines],
        [HBM] * 3,
        [
            pltpu.VMEM(many, jnp.float32),
            pltpu.VMEM(many, jnp.float32),
            pltpu.VMEM((members, levels, 8, cols), jnp.float32),
            pltpu.SemaphoreType.DMA((members, 3)),
        ],
        limit=60,
    )(pressure, east_wind, north_wind)
    west, east, both = exchange(columns, edge_rows)
    hcols, hrows, *weights = call(
        weight_kernel,
        [(rows, cols), (2, levels, cols)] + [field] * 9 + [many, vertical_wind.shape],
        [VMEM, HBM, HBM, SMEM],
        [pltpu.SemaphoreType.DMA((2,))],
        limit=24,
    )(sound_squared, north_wind, vertical_wind, thickness)
    *weights, north_wind, vertical_wind = weights
    sums, columns, edge_rows = call(
        main_kernel,
        [(members, 3, rows, cols), plane, lines],
        [VMEM] * 5 + [SMEM] + [VMEM] * 12,
        [pltpu.VMEM(many, jnp.float32)] * 4,
        limit=32,
    )(
        pressure, east_wind, north_wind, vertical_wind, sound_squared, thickness, *weights, west, east, both
    )
    west, east, both = exchange(columns, edge_rows)
    quarters = call(
        edge_kernel,
        [(members, 3, height, cols)] * ranks,
        [VMEM] * 6,
        [pltpu.VMEM((members, 3, rows, cols), jnp.float32)],
    )(sums, west, east, both, hcols, hrows)
    quarters = [
        permuted(x, "mem", lambda i, d=d: i ^ d) if d else x for d, x in enumerate(quarters)
    ]
    (stats,) = call(stats_kernel, [part], [VMEM] * ranks)(*quarters)
    tiles = [permuted(stats, "ty", lambda i, j=j: i ^ j) if j else stats for j in range(height_count)]
    chosen = call(
        functools.partial(select_kernel, width), [part] * width, [SMEM] + [VMEM] * height_count
    )(owner_map, *tiles)
    routed = [permuted(x, "tx", lambda i, d=d: i ^ d) if d else x for d, x in enumerate(chosen)]
    (result,) = call(
        functools.partial(pick_kernel, height_count), [(1, 1) + part], [SMEM] + [VMEM] * width
    )(owner_map, *routed)
    return result


def solution(mesh):
    placed = (
        P("mem", None, "ty", "tx"),
        P("mem", None, "ty", "tx"),
        P("mem", None, "ty", "tx"),
        P("mem", None, "ty", "tx"),
        P(None, "ty", "tx"),
        P(),
        P(),
    )
    return jax.shard_map(
        local,
        mesh=mesh,
        in_specs=placed,
        out_specs=P("ty", "tx", None, "mem", None),
        check_vma=False,
    )
```

```python
import functools

import jax
import jax.numpy as jnp
from jax import lax
from jax.experimental import pallas as pl
from jax.experimental.pallas import tpu as pltpu
from jax.sharding import PartitionSpec as P


HORIZ = 0.35
VERT = 1.5
STEP_A = 50
STEP_P = 10
STEP_B = 25
STEP_S = 25
PACK_LIMIT = 16
PREP_LIMIT = 24

VMEM = pl.BlockSpec(memory_space=pltpu.VMEM)
SMEM = pl.BlockSpec(memory_space=pltpu.SMEM)
HBM = pl.BlockSpec(memory_space=pltpu.HBM)


def divisor(count, most):
    return max(d for d in range(1, most + 1) if count % d == 0)


def lanes_of(shape):
    return lax.broadcasted_iota(jnp.int32, shape, len(shape) - 1)


def rows_of(shape):
    return lax.broadcasted_iota(jnp.int32, shape, len(shape) - 2)


def west_roll(x):
    return pltpu.roll(x, 1, 1)


def east_roll(x):
    return pltpu.roll(x, x.shape[1] - 1, 1)


def south_roll(x):
    return pltpu.roll(x, 1, 0)


def north_roll(x):
    return pltpu.roll(x, x.shape[0] - 1, 0)


def sides(far_ref, near_ref):
    odd = lax.axis_index("tx") % 2 == 1
    far = [far_ref[m] for m in range(far_ref.shape[0])]
    near = [near_ref[m] for m in range(near_ref.shape[0])]
    west = [jnp.where(odd, a, b) for a, b in zip(near, far)]
    east = [jnp.where(odd, b, a) for a, b in zip(near, far)]
    return west, east


def pack_kernel(p_hbm, u_hbm, v_hbm, cols_ref, rows_ref, p_ref, u_ref, v_s, sems):
    members, levels, rows, cols = p_ref.shape
    copies = []
    for m in range(members):
        pair = [
            pltpu.make_async_copy(p_hbm.at[m], p_ref.at[m], sems.at[m, 0]),
            pltpu.make_async_copy(u_hbm.at[m], u_ref.at[m], sems.at[m, 1]),
            pltpu.make_async_copy(v_hbm.at[m, :, 0:8], v_s.at[m], sems.at[m, 2]),
        ]
        for copy in pair:
            copy.start()
        copies.append(pair)
    lane = lanes_of((rows, cols))
    for m in range(members):
        for copy in copies[m]:
            copy.wait()
        packed = jnp.zeros((rows, cols), jnp.float32)
        for k in range(levels):
            p = p_ref[m, k]
            z = u_ref[m, k] - HORIZ * p
            edge = pltpu.roll(jnp.where(lane == cols - 1, p, z), 2 * k + 1, 1)
            packed = jnp.where(lane >= 2 * k, edge, packed)
            rows_ref[0, m, k : k + 1, :] = p[rows - 1 : rows, :]
            rows_ref[1, m, k : k + 1, :] = v_s[m, k, 0:1, :] - HORIZ * p[0:1, :]
        cols_ref[m] = packed


def prepare_kernel(
    c_ref, p_ref, u0_ref, v_hbm, w_hbm, th_ref, owner_ref,
    hcols_ref, hrows_ref, hth_ref, masks_ref,
    e_s, inv_s, s_s, g_s, h_s, hw_s, he_s, hs_s, hn_s, part_ref, u_ref, v_ref, w_ref, sems,
):
    members, levels, rows, cols = part_ref.shape
    copies = [
        pltpu.make_async_copy(source.at[m], target.at[m], sems.at[i, m])
        for i, (source, target) in enumerate([(v_hbm, v_ref), (w_hbm, w_ref)])
        for m in range(members)
    ]
    for copy in copies:
        copy.start()
    inner = levels - 1
    shape = (rows, cols)
    lane = lanes_of(shape)
    row = rows_of(shape)
    first_lane, last_lane = lane == 0, lane == cols - 1
    first_row, last_row = row == 0, row == rows - 1
    zero = jnp.zeros(shape, jnp.float32)
    vsq = VERT * VERT

    height, width = lax.axis_size("ty"), lax.axis_size("tx")
    my_row, my_column = lax.axis_index("ty"), lax.axis_index("tx")
    mask = (8, cols)
    for j in range(height):
        for d in range(width):
            here = owner_ref[(my_row ^ j) * width + my_column] == my_row * width + (my_column ^ d)
            masks_ref[j * width + d] = jnp.full(mask, jnp.where(here, 1.0, 0.0), jnp.float32)
    for d in range(width):
        here = jnp.float32(0.0)
        for j in range(height):
            mine = owner_ref[j * width + (my_column ^ d)] == my_row * width + my_column
            here = jnp.where(mine, 1.0, here)
        masks_ref[height * width + d] = jnp.full(mask, here, jnp.float32)

    for ref in (e_s, inv_s, s_s):
        ref[0] = zero

    step = divisor(inner, STEP_A)

    def factor(chunk, carry):
        e_prev, s_prev, c_here = carry
        for sub in range(step):
            i = chunk * step + sub
            c_next = c_ref[i + 1]
            b_next = vsq * c_next
            pivot = (1.0 + b_next) + (vsq * c_here) * (1.0 - e_prev)
            inv = 1.0 / pivot
            s_prev = VERT * (th_ref[i + 1] * c_next - th_ref[i] * c_here) + e_prev * s_prev
            e_prev = b_next * inv
            e_s[i + 1] = e_prev
            inv_s[i + 1] = inv
            s_s[i + 1] = s_prev * inv
            c_here = c_next
        return e_prev, s_prev, c_here

    lax.fori_loop(0, inner // step, factor, (zero, zero, c_ref[0]))

    def weights(k, y_above, y_here):
        g = th_ref[k] + VERT * (y_above - y_here)
        h = g * (HORIZ * c_ref[k])
        g_s[k] = g - (2 * HORIZ) * h
        h_s[k] = h
        h35 = HORIZ * h
        hw_s[k] = jnp.where(first_lane, 0.0, west_roll(h))
        he_s[k] = jnp.where(last_lane, 0.0, east_roll(h35))
        hs_s[k] = jnp.where(first_row, 0.0, south_roll(h))
        hn_s[k] = jnp.where(last_row, 0.0, north_roll(h35))
        hrows_ref[0, pl.ds(k, 1), :] = h35[0:1, :]
        hrows_ref[1, pl.ds(k, 1), :] = h[rows - 1 : rows, :]
        hrows_ref[2, pl.ds(k, 1), :] = jnp.full((1, cols), HORIZ * th_ref[k], jnp.float32)
        return jnp.where(last_lane, -h, h35)

    def adjoint(chunk, carry):
        y_above, packed = carry
        packed = pltpu.roll(packed, 2 * step, 1)
        for sub in range(step):
            i = inner - 1 - (chunk * step + sub)
            y_here = s_s[i + 1] + e_s[i + 1] * y_above
            s_s[i + 1] = y_here
            edge = weights(i + 1, y_above, y_here)
            place = 2 * (step - 1 - sub)
            packed = jnp.where(lane < place + 2, pltpu.roll(edge, place + 1, 1), packed)
            y_above = y_here
        return y_above, packed

    y_low, packed = lax.fori_loop(0, inner // step, adjoint, (zero, zero))
    edge = weights(0, y_low, zero)
    hcols_ref[...] = jnp.where(lane < 2, pltpu.roll(edge, 1, 1), pltpu.roll(packed, 2, 1))
    hth = jnp.zeros(mask, jnp.float32)
    for k in range(levels):
        hth = jnp.where(lanes_of(mask) == 2 * k + 1, HORIZ * th_ref[k], hth)
    hth_ref[...] = hth

    for copy in copies[:members]:
        copy.wait()
    step1 = divisor(levels, STEP_P)

    def first_winds(chunk, carry):
        for sub in range(step1):
            k = chunk * step1 + sub
            c35 = HORIZ * c_ref[k]
            for m in range(members):
                p = p_ref[m, k]
                q = HORIZ * p
                zu = u0_ref[m, k] - q
                zv = v_ref[m, k] - q
                u1 = zu + jnp.where(first_lane, 0.0, west_roll(q))
                v1 = zv + jnp.where(first_row, 0.0, south_roll(q))
                u_ref[m, k] = u1
                v_ref[m, k] = v1
                zu_east = jnp.where(last_lane, 0.0, east_roll(zu))
                zv_north = jnp.where(last_row, 0.0, north_roll(zv))
                div = ((zu_east + q) - u1) + ((zv_north + q) - v1)
                part_ref[m, k] = p - c35 * div
        return carry

    lax.fori_loop(0, levels // step1, first_winds, 0)
    for copy in copies[members:]:
        copy.wait()


def solve_kernel(
    c_ref, part_ref, u_ref, v_ref, w_ref, e_s, inv_s, far_ref, near_ref, from_rows,
    cols_ref, rows_ref, p1_ref, zu_ref, zv_ref, w1_ref,
):
    members, levels, rows, cols = part_ref.shape
    group = 8
    groups = rows // group
    gshape = (group, cols)
    slices = [slice(g * group, (g + 1) * group) for g in range(groups)]
    lane, row = lanes_of(gshape), rows_of(gshape)
    zero = jnp.zeros(gshape, jnp.float32)
    at_first = jnp.where(lane == 0, 1.0, 0.0)
    signed = jnp.where(lane == cols - 1, -1.0, at_first)
    even = lane % 2 == 0
    from_west, from_east = sides(far_ref, near_ref)
    halo = []
    for m in range(members):
        for rs in slices:
            mixed = jnp.where(even, east_roll(from_east[m][rs]), HORIZ * west_roll(from_west[m][rs]))
            halo.append(east_roll(mixed))
    step1 = divisor(levels, STEP_B)

    def upward(chunk, carry):
        part_prev, v_prev, halo = (list(x) for x in carry)
        for sub in range(step1):
            k = chunk * step1 + sub
            below = jnp.maximum(k - 1, 0)
            for g, rs in enumerate(slices):
                c35 = HORIZ * c_ref[k, rs]
                e = e_s[below, rs]
                for m in range(members):
                    at = m * groups + g
                    edge = halo[at] if sub == 0 else pltpu.roll(halo[at], cols - 2 * sub, 1)
                    zu_ref[m, k, rs] = u_ref[m, k, rs] + edge * at_first
                    delta = edge * signed
                    if g == 0:
                        delta = delta + jnp.where(row == 0, HORIZ * from_rows[0, m, pl.ds(k, 1), :], 0.0)
                    if g == groups - 1:
                        delta = delta - jnp.where(row == group - 1, from_rows[1, m, pl.ds(k, 1), :], 0.0)
                    part = part_ref[m, k, rs] + c35 * delta
                    p1_ref[m, k, rs] = part
                    rhs = w_ref[m, below, rs] - VERT * (part - part_prev[at])
                    v_new = rhs + e * v_prev[at]
                    w1_ref[m, k, rs] = v_new
                    v_prev[at] = v_new
                    part_prev[at] = part
        halo = [pltpu.roll(x, cols - 2 * step1, 1) for x in halo]
        return tuple(part_prev), tuple(v_prev), tuple(halo)

    zeros = (zero,) * (members * groups)
    lax.fori_loop(0, levels // step1, upward, (zeros, zeros, tuple(halo)))

    last = lane == cols - 1
    for g, rs in enumerate(slices):

        def downward(chunk, carry, g=g, rs=rs):
            ws, packs = list(carry[0]), list(carry[1])
            base = levels - step1 - chunk * step1
            for sub in range(step1):
                k = base + (step1 - 1 - sub)
                inv, e = inv_s[k, rs], e_s[k, rs]
                c15 = VERT * c_ref[k, rs]
                for m in range(members):
                    w = ws[m]
                    w_low = w1_ref[m, k, rs] * inv + e * w
                    w1_ref[m, k, rs] = w_low
                    p = p1_ref[m, k, rs] - c15 * (w - w_low)
                    p1_ref[m, k, rs] = p
                    q = HORIZ * p
                    zu = zu_ref[m, k, rs] - q
                    zu_ref[m, k, rs] = zu
                    v1 = v_ref[m, k, rs]
                    if g == 0:
                        v1 = v1 + jnp.where(row == 0, HORIZ * from_rows[0, m, pl.ds(k, 1), :], 0.0)
                    zv = v1 - q
                    zv_ref[m, k, rs] = zv
                    place = 2 * (step1 - 1 - sub)
                    edge = pltpu.roll(jnp.where(last, p, zu), place + 1, 1)
                    if sub == 0:
                        packs[m] = pltpu.roll(packs[m], 2 * step1, 1)
                    packs[m] = jnp.where(lane < place + 2, edge, packs[m])
                    if g == groups - 1:
                        rows_ref[0, m, pl.ds(k, 1), :] = p[group - 1 : group, :]
                    if g == 0:
                        rows_ref[1, m, pl.ds(k, 1), :] = zv[0:1, :]
                    ws[m] = w_low
            return tuple(ws), tuple(packs)

        init = ((zero,) * members,) * 2
        _, packs = lax.fori_loop(0, levels // step1, downward, init)
        for m in range(members):
            cols_ref[m, rs] = packs[m]


def sum_kernel(
    p1_ref, zu_ref, zv_ref, w1_ref, th_ref, s_s, g_s, h_s, hw_s, he_s, hs_s, hn_s, sums_ref, keep_s
):
    members, levels, rows, cols = p1_ref.shape
    group = 8
    gshape = (group, cols)
    glane = lanes_of(gshape)
    gzero = jnp.zeros(gshape, jnp.float32)
    step1 = divisor(levels, STEP_S)
    for r in range(rows // group):
        rs = slice(r * group, (r + 1) * group)

        def downward(chunk, carry, rs=rs):
            state = [list(x) for x in carry]
            base = levels - step1 - chunk * step1
            for sub in range(step1):
                k = base + (step1 - 1 - sub)
                g, h, th = g_s[k, rs], h_s[k, rs], th_ref[k]
                y = s_s[k, rs]
                hw, he, hs, hn = hw_s[k, rs], he_s[k, rs], hs_s[k, rs], hn_s[k, rs]
                for m in range(members):
                    mass, ps, us, vs, ce, cw, cn, cs = state[m]
                    p, zu, zv = p1_ref[m, k, rs], zu_ref[m, k, rs], zv_ref[m, k, rs]
                    mass = mass + ((g * p + y * w1_ref[m, k, rs]) + h * (zu + zv))
                    ps = ps + th * p
                    us = us + th * zu
                    vs = vs + th * zv
                    ce = ce + hw * zu
                    cw = cw + he * p
                    cn = cn + hs * zv
                    cs = cs + hn * p
                    state[m] = [mass, ps, us, vs, ce, cw, cn, cs]
            return tuple(tuple(x) for x in state)

        out = lax.fori_loop(0, levels // step1, downward, ((gzero,) * 8,) * members)
        for m in range(members):
            mass, ps, us, vs, ce, cw, cn, cs = out[m]
            sums_ref[m, 0, rs] = mass - east_roll(ce) + west_roll(cw)
            sums_ref[m, 1, rs] = us + jnp.where(glane == 0, 0.0, HORIZ * west_roll(ps))
            sums_ref[m, 2, rs] = vs
            keep_s[m, 0, rs] = ps
            keep_s[m, 1, rs] = cn
            keep_s[m, 2, rs] = cs
    row = rows_of((rows, cols))
    for m in range(members):
        ps, cn, cs = keep_s[m, 0], keep_s[m, 1], keep_s[m, 2]
        sums_ref[m, 0] = sums_ref[m, 0] - north_roll(cn) + south_roll(cs)
        sums_ref[m, 2] = sums_ref[m, 2] + jnp.where(row == 0, 0.0, HORIZ * south_roll(ps))


def edge_kernel(sums_ref, far_ref, near_ref, from_rows, hcols_ref, hrows_ref, hth_ref, *rest):
    outs, total_s = rest[:-1], rest[-1]
    from_west, from_east = sides(far_ref, near_ref)
    members, _, rows, cols = sums_ref.shape
    levels = hrows_ref.shape[1]
    height = rows // len(outs)
    mine = lax.axis_index("mem")
    lane = lanes_of((rows, cols))
    row = rows_of((rows, cols))
    even = lane % 2 == 0
    used = lane < 2 * levels
    hth = jnp.concatenate([hth_ref[...]] * (rows // 8), axis=0)
    for m in range(members):
        west = west_roll(from_west[m])
        products = jnp.where(used, hcols_ref[...] * jnp.where(even, east_roll(from_east[m]), west), 0.0)
        at_east = jnp.sum(jnp.where(even, products, 0.0), axis=1, keepdims=True)
        at_west = jnp.sum(jnp.where(even, 0.0, products), axis=1, keepdims=True)
        u_west = jnp.sum(hth * west, axis=1, keepdims=True)
        at_south = jnp.sum(hrows_ref[0] * from_rows[0, m], axis=0, keepdims=True)
        at_north = jnp.sum(hrows_ref[1] * from_rows[1, m], axis=0, keepdims=True)
        v_south = jnp.sum(hrows_ref[2] * from_rows[0, m], axis=0, keepdims=True)
        mass = sums_ref[m, 0] + jnp.where(lane == 0, at_west, 0.0) + jnp.where(lane == cols - 1, at_east, 0.0)
        mass = mass + jnp.where(row == 0, at_south, 0.0) - jnp.where(row == rows - 1, at_north, 0.0)
        total_s[m, 0] = mass
        total_s[m, 1] = sums_ref[m, 1] + jnp.where(lane == 0, u_west, 0.0)
        total_s[m, 2] = sums_ref[m, 2] + jnp.where(row == 0, v_south, 0.0)
    for d, out_ref in enumerate(outs):
        start = pl.multiple_of((mine ^ d) * height, height)
        out_ref[...] = total_s[:, :, pl.ds(start, height), :]


def stats_kernel(*refs):
    ins, out_ref = refs[:-1], refs[-1]
    members, fields = ins[0].shape[:2]
    count = len(ins) * members
    for f in range(fields):
        values = [ref[m, f] for ref in ins for m in range(members)]
        mean = functools.reduce(jnp.add, values) / count
        square = functools.reduce(jnp.add, [(v - mean) * (v - mean) for v in values]) / (count - 1)
        out_ref[f] = mean
        out_ref[fields + f] = square


def select_kernel(width, masks_ref, *refs):
    tiles, outs = refs[:-width], refs[-width:]
    for d, out_ref in enumerate(outs):
        for f in range(out_ref.shape[0]):
            value = tiles[0][f]
            for j in range(1, len(tiles)):
                value = jnp.where(masks_ref[j * width + d] > 0.5, tiles[j][f], value)
            out_ref[f] = value


def pick_kernel(masks_ref, *refs):
    ins, out_ref = refs[:-1], refs[-1]
    width = len(ins)
    base = masks_ref.shape[0] - width
    for f in range(ins[0].shape[0]):
        value = ins[0][f]
        for d in range(1, width):
            value = jnp.where(masks_ref[base + d] > 0.5, ins[d][f], value)
        out_ref[0, 0, f] = value


def call(kernel, outs, in_specs, scratch=(), limit=16):
    return pl.pallas_call(
        kernel,
        out_shape=[jax.ShapeDtypeStruct(s, jnp.float32) for s in outs],
        in_specs=in_specs,
        out_specs=[VMEM] * len(outs),
        scratch_shapes=list(scratch),
        compiler_params=pltpu.CompilerParams(vmem_limit_bytes=limit * 1024 * 1024),
    )


def permuted(block, axis, source):
    count = lax.axis_size(axis)
    return lax.ppermute(block, axis, [(source(i) % count, i) for i in range(count)])


def exchange(columns, edge_rows):
    far = permuted(columns, "tx", lambda i: i + 1 if i % 2 else i - 1)
    near = permuted(columns, "tx", lambda i: i ^ 1)
    if lax.axis_size("ty") <= 2:
        both = permuted(edge_rows, "ty", lambda i: i - 1)
    else:
        south = permuted(edge_rows[0], "ty", lambda i: i - 1)
        north = permuted(edge_rows[1], "ty", lambda i: i + 1)
        both = jnp.stack([south, north])
    return far, near, both


def steps(pressure, east_wind, north_wind, vertical_wind, sound_squared, thickness, owner_map):
    members, levels, rows, cols = pressure.shape
    ranks, height_count, width = (lax.axis_size(a) for a in ("mem", "ty", "tx"))
    height = rows // ranks
    plane = (members, rows, cols)
    many = (members, levels, rows, cols)
    field = (levels, rows, cols)
    lines = (2, members, levels, cols)
    part = (6, height, cols)
    pressure, east_wind, north_wind, vertical_wind = (
        pltpu.with_memory_space_constraint(x, pltpu.HBM)
        for x in (pressure, east_wind, north_wind, vertical_wind)
    )
    columns, edge_rows, p0, u0 = call(
        pack_kernel,
        [plane, lines, many, many],
        [HBM] * 3,
        [
            pltpu.VMEM((members, levels, 8, cols), jnp.float32),
            pltpu.SemaphoreType.DMA((members, 3)),
        ],
        limit=PACK_LIMIT,
    )(pressure, east_wind, north_wind)
    far, near, both = exchange(columns, edge_rows)
    hcols, hrows, hth, masks, e, inv, *weights, part0, u0, v0, w0 = call(
        prepare_kernel,
        [
            (rows, cols),
            (3, levels, cols),
            (8, cols),
            (height_count * width + width, 8, cols),
            *[field] * 9,
            *[many] * 3,
            vertical_wind.shape,
        ],
        [VMEM, VMEM, VMEM, HBM, HBM, SMEM, SMEM],
        [pltpu.SemaphoreType.DMA((2, members))],
        limit=PREP_LIMIT,
    )(sound_squared, p0, u0, north_wind, vertical_wind, thickness, owner_map)
    columns, edge_rows, p1, zu, zv, w1 = call(
        solve_kernel, [plane, lines, *[many] * 4], [VMEM] * 10
    )(sound_squared, part0, u0, v0, w0, e, inv, far, near, both)
    far, near, both = exchange(columns, edge_rows)
    (sums,) = call(
        sum_kernel,
        [(members, 3, rows, cols)],
        [VMEM] * 4 + [SMEM] + [VMEM] * 7,
        [pltpu.VMEM((members, 3, rows, cols), jnp.float32)],
    )(p1, zu, zv, w1, thickness, *weights)
    quarters = call(
        edge_kernel,
        [(members, 3, height, cols)] * ranks,
        [VMEM] * 7,
        [pltpu.VMEM((members, 3, rows, cols), jnp.float32)],
    )(sums, far, near, both, hcols, hrows, hth)
    quarters = [
        permuted(x, "mem", lambda i, d=d: i ^ d) if d else x for d, x in enumerate(quarters)
    ]
    (stats,) = call(stats_kernel, [part], [VMEM] * ranks)(*quarters)
    tiles = [
        permuted(stats, "ty", lambda i, j=j: i ^ j) if j else stats
        for j in range(height_count)
    ]
    chosen = call(
        functools.partial(select_kernel, width), [part] * width, [VMEM] * (1 + height_count)
    )(masks, *tiles)
    routed = [permuted(x, "tx", lambda i, d=d: i ^ d) if d else x for d, x in enumerate(chosen)]
    (result,) = call(pick_kernel, [(1, 1) + part], [VMEM] * (1 + width))(masks, *routed)
    return result


def solution(mesh):
    placed = (
        P("mem", None, "ty", "tx"),
        P("mem", None, "ty", "tx"),
        P("mem", None, "ty", "tx"),
        P("mem", None, "ty", "tx"),
        P(None, "ty", "tx"),
        P(),
        P(),
    )
    return jax.shard_map(
        steps,
        mesh=mesh,
        in_specs=placed,
        out_specs=P("ty", "tx", None, "mem", None),
        check_vma=False,
    )
```

```python
import functools

import jax
import jax.numpy as jnp
from jax import lax
from jax.experimental import pallas as pl
from jax.experimental.pallas import tpu as pltpu
from jax.sharding import PartitionSpec as P


HORIZ = 0.35
VERT = 1.5
STEP_A = 8
STEP_P = 10
STEP_B = 25
STEP_D = 25
STEP_S = 25
PACK_LIMIT = 16
PREP_LIMIT = 24

VMEM = pl.BlockSpec(memory_space=pltpu.VMEM)
SMEM = pl.BlockSpec(memory_space=pltpu.SMEM)
HBM = pl.BlockSpec(memory_space=pltpu.HBM)


def divisor(count, most):
    return max(d for d in range(1, most + 1) if count % d == 0)


def lanes_of(shape):
    return lax.broadcasted_iota(jnp.int32, shape, len(shape) - 1)


def rows_of(shape):
    return lax.broadcasted_iota(jnp.int32, shape, len(shape) - 2)


def west_roll(x):
    return pltpu.roll(x, 1, 1)


def east_roll(x):
    return pltpu.roll(x, x.shape[1] - 1, 1)


def south_roll(x):
    return pltpu.roll(x, 1, 0)


def north_roll(x):
    return pltpu.roll(x, x.shape[0] - 1, 0)


def sides(far_ref, near_ref):
    odd = lax.axis_index("tx") % 2 == 1
    far = [far_ref[m] for m in range(far_ref.shape[0])]
    near = [near_ref[m] for m in range(near_ref.shape[0])]
    west = [jnp.where(odd, a, b) for a, b in zip(near, far)]
    east = [jnp.where(odd, b, a) for a, b in zip(near, far)]
    return west, east


def pack_kernel(p_hbm, u_hbm, v_hbm, cols_ref, rows_ref, p_ref, u_ref, v_s, sems):
    members, levels, rows, cols = p_ref.shape
    copies = []
    for m in range(members):
        pair = [
            pltpu.make_async_copy(p_hbm.at[m], p_ref.at[m], sems.at[m, 0]),
            pltpu.make_async_copy(u_hbm.at[m], u_ref.at[m], sems.at[m, 1]),
            pltpu.make_async_copy(v_hbm.at[m, :, 0:8], v_s.at[m], sems.at[m, 2]),
        ]
        for copy in pair:
            copy.start()
        copies.append(pair)
    lane = lanes_of((rows, cols))
    for m in range(members):
        for copy in copies[m]:
            copy.wait()
        packed = jnp.zeros((rows, cols), jnp.float32)
        for k in range(levels):
            p = p_ref[m, k]
            z = u_ref[m, k] - HORIZ * p
            edge = pltpu.roll(jnp.where(lane == cols - 1, p, z), 2 * k + 1, 1)
            packed = jnp.where(lane >= 2 * k, edge, packed)
            rows_ref[0, m, k : k + 1, :] = p[rows - 1 : rows, :]
            rows_ref[1, m, k : k + 1, :] = v_s[m, k, 0:1, :] - HORIZ * p[0:1, :]
        cols_ref[m] = packed


def prepare_kernel(
    c_ref, p_ref, u0_ref, v_hbm, w_hbm, th_ref, owner_ref,
    hcols_ref, hrows_ref, hth_ref, masks_ref,
    e_s, inv_s, s_s, g_s, h_s, hw_s, he_s, hs_s, hn_s, part_ref, u_ref, v_ref, w_ref, sems,
):
    members, levels, rows, cols = part_ref.shape
    copies = [
        pltpu.make_async_copy(source.at[m], target.at[m], sems.at[i, m])
        for i, (source, target) in enumerate([(v_hbm, v_ref), (w_hbm, w_ref)])
        for m in range(members)
    ]
    for copy in copies:
        copy.start()
    inner = levels - 1
    shape = (rows, cols)
    lane = lanes_of(shape)
    row = rows_of(shape)
    first_lane, last_lane = lane == 0, lane == cols - 1
    first_row, last_row = row == 0, row == rows - 1
    zero = jnp.zeros(shape, jnp.float32)
    vsq = VERT * VERT

    height, width = lax.axis_size("ty"), lax.axis_size("tx")
    my_row, my_column = lax.axis_index("ty"), lax.axis_index("tx")
    mask = (8, cols)
    for j in range(height):
        for d in range(width):
            here = owner_ref[(my_row ^ j) * width + my_column] == my_row * width + (my_column ^ d)
            masks_ref[j * width + d] = jnp.full(mask, jnp.where(here, 1.0, 0.0), jnp.float32)
    for d in range(width):
        here = jnp.float32(0.0)
        for j in range(height):
            mine = owner_ref[j * width + (my_column ^ d)] == my_row * width + my_column
            here = jnp.where(mine, 1.0, here)
        masks_ref[height * width + d] = jnp.full(mask, here, jnp.float32)

    for ref in (e_s, inv_s, s_s):
        ref[0] = zero

    step = divisor(inner, STEP_A)

    def factor(chunk, carry):
        e_prev, s_prev, c_here = carry
        for sub in range(step):
            i = chunk * step + sub
            c_next = c_ref[i + 1]
            b_next = vsq * c_next
            pivot = (1.0 + b_next) + (vsq * c_here) * (1.0 - e_prev)
            inv = 1.0 / pivot
            s_prev = VERT * (th_ref[i + 1] * c_next - th_ref[i] * c_here) + e_prev * s_prev
            e_prev = b_next * inv
            e_s[i + 1] = e_prev
            inv_s[i + 1] = inv
            s_s[i + 1] = s_prev * inv
            c_here = c_next
        return e_prev, s_prev, c_here

    lax.fori_loop(0, inner // step, factor, (zero, zero, c_ref[0]))

    def weights(k, y_above, y_here):
        g = th_ref[k] + VERT * (y_above - y_here)
        h = g * (HORIZ * c_ref[k])
        g_s[k] = g - (2 * HORIZ) * h
        h_s[k] = h
        h35 = HORIZ * h
        hw_s[k] = jnp.where(first_lane, 0.0, west_roll(h))
        he_s[k] = jnp.where(last_lane, 0.0, east_roll(h35))
        hs_s[k] = jnp.where(first_row, 0.0, south_roll(h))
        hn_s[k] = jnp.where(last_row, 0.0, north_roll(h35))
        hrows_ref[0, pl.ds(k, 1), :] = h35[0:1, :]
        hrows_ref[1, pl.ds(k, 1), :] = h[rows - 1 : rows, :]
        hrows_ref[2, pl.ds(k, 1), :] = jnp.full((1, cols), HORIZ * th_ref[k], jnp.float32)
        return jnp.where(last_lane, -h, h35)

    def adjoint(chunk, carry):
        y_above, packed = carry
        packed = pltpu.roll(packed, 2 * step, 1)
        for sub in range(step):
            i = inner - 1 - (chunk * step + sub)
            y_here = s_s[i + 1] + e_s[i + 1] * y_above
            s_s[i + 1] = y_here
            edge = weights(i + 1, y_above, y_here)
            place = 2 * (step - 1 - sub)
            packed = jnp.where(lane < place + 2, pltpu.roll(edge, place + 1, 1), packed)
            y_above = y_here
        return y_above, packed

    y_low, packed = lax.fori_loop(0, inner // step, adjoint, (zero, zero))
    edge = weights(0, y_low, zero)
    hcols_ref[...] = jnp.where(lane < 2, pltpu.roll(edge, 1, 1), pltpu.roll(packed, 2, 1))
    hth = jnp.zeros(mask, jnp.float32)
    for k in range(levels):
        hth = jnp.where(lanes_of(mask) == 2 * k + 1, HORIZ * th_ref[k], hth)
    hth_ref[...] = hth

    for copy in copies[:members]:
        copy.wait()
    step1 = divisor(levels, STEP_P)

    def first_winds(chunk, carry):
        for sub in range(step1):
            k = chunk * step1 + sub
            c35 = HORIZ * c_ref[k]
            for m in range(members):
                p = p_ref[m, k]
                q = HORIZ * p
                zu = u0_ref[m, k] - q
                zv = v_ref[m, k] - q
                u1 = zu + jnp.where(first_lane, 0.0, west_roll(q))
                v1 = zv + jnp.where(first_row, 0.0, south_roll(q))
                u_ref[m, k] = u1
                v_ref[m, k] = v1
                zu_east = jnp.where(last_lane, 0.0, east_roll(zu))
                zv_north = jnp.where(last_row, 0.0, north_roll(zv))
                div = ((zu_east + q) - u1) + ((zv_north + q) - v1)
                part_ref[m, k] = p - c35 * div
        return carry

    lax.fori_loop(0, levels // step1, first_winds, 0)
    for copy in copies[members:]:
        copy.wait()


def solve_kernel(
    c_ref, part_ref, u_ref, v_ref, w_ref, e_s, inv_s, far_ref, near_ref, from_rows,
    cols_ref, rows_ref, p1_ref, zu_ref, zv_ref, w1_ref,
):
    members, levels, rows, cols = part_ref.shape
    group = 8
    groups = rows // group
    gshape = (group, cols)
    slices = [slice(g * group, (g + 1) * group) for g in range(groups)]
    lane, row = lanes_of(gshape), rows_of(gshape)
    zero = jnp.zeros(gshape, jnp.float32)
    at_first = jnp.where(lane == 0, 1.0, 0.0)
    signed = jnp.where(lane == cols - 1, -1.0, at_first)
    even = lane % 2 == 0
    from_west, from_east = sides(far_ref, near_ref)
    halo = []
    for m in range(members):
        for rs in slices:
            mixed = jnp.where(even, east_roll(from_east[m][rs]), HORIZ * west_roll(from_west[m][rs]))
            halo.append(east_roll(mixed))
    step1 = divisor(levels, STEP_B)

    def upward(chunk, carry):
        part_prev, v_prev, halo = (list(x) for x in carry)
        for sub in range(step1):
            k = chunk * step1 + sub
            below = jnp.maximum(k - 1, 0)
            for g, rs in enumerate(slices):
                c35 = HORIZ * c_ref[k, rs]
                e = e_s[below, rs]
                for m in range(members):
                    at = m * groups + g
                    edge = halo[at] if sub == 0 else pltpu.roll(halo[at], cols - 2 * sub, 1)
                    zu_ref[m, k, rs] = u_ref[m, k, rs] + edge * at_first
                    delta = edge * signed
                    if g == 0:
                        delta = delta + jnp.where(row == 0, HORIZ * from_rows[0, m, pl.ds(k, 1), :], 0.0)
                    if g == groups - 1:
                        delta = delta - jnp.where(row == group - 1, from_rows[1, m, pl.ds(k, 1), :], 0.0)
                    part = part_ref[m, k, rs] + c35 * delta
                    p1_ref[m, k, rs] = part
                    rhs = w_ref[m, below, rs] - VERT * (part - part_prev[at])
                    v_new = rhs + e * v_prev[at]
                    w1_ref[m, k, rs] = v_new
                    v_prev[at] = v_new
                    part_prev[at] = part
        halo = [pltpu.roll(x, cols - 2 * step1, 1) for x in halo]
        return tuple(part_prev), tuple(v_prev), tuple(halo)

    zeros = (zero,) * (members * groups)
    lax.fori_loop(0, levels // step1, upward, (zeros, zeros, tuple(halo)))

    last = lane == cols - 1

    def downward(chunk, carry):
        ws, packs = list(carry[0]), list(carry[1])
        base = levels - step2 - chunk * step2
        for sub in range(step2):
            place = 2 * (step2 - 1 - sub)
            k = base + (step2 - 1 - sub)
            for g, rs in enumerate(slices):
                inv, e = inv_s[k, rs], e_s[k, rs]
                c15 = VERT * c_ref[k, rs]
                for m in range(members):
                    at = m * groups + g
                    w = ws[at]
                    w_low = w1_ref[m, k, rs] * inv + e * w
                    w1_ref[m, k, rs] = w_low
                    p = p1_ref[m, k, rs] - c15 * (w - w_low)
                    p1_ref[m, k, rs] = p
                    q = HORIZ * p
                    zu = zu_ref[m, k, rs] - q
                    zu_ref[m, k, rs] = zu
                    v1 = v_ref[m, k, rs]
                    if g == 0:
                        v1 = v1 + jnp.where(row == 0, HORIZ * from_rows[0, m, pl.ds(k, 1), :], 0.0)
                    zv = v1 - q
                    zv_ref[m, k, rs] = zv
                    edge = pltpu.roll(jnp.where(last, p, zu), place + 1, 1)
                    if sub == 0:
                        packs[at] = pltpu.roll(packs[at], 2 * step2, 1)
                    packs[at] = jnp.where(lane < place + 2, edge, packs[at])
                    if g == groups - 1:
                        rows_ref[0, m, pl.ds(k, 1), :] = p[group - 1 : group, :]
                    if g == 0:
                        rows_ref[1, m, pl.ds(k, 1), :] = zv[0:1, :]
                    ws[at] = w_low
        return tuple(ws), tuple(packs)

    step2 = divisor(levels, STEP_D)
    _, packs = lax.fori_loop(0, levels // step2, downward, (zeros, zeros))
    for m in range(members):
        for g, rs in enumerate(slices):
            cols_ref[m, rs] = packs[m * groups + g]


def sum_kernel(
    p1_ref, zu_ref, zv_ref, w1_ref, th_ref, s_s, g_s, h_s, hw_s, he_s, hs_s, hn_s, sums_ref, keep_s
):
    members, levels, rows, cols = p1_ref.shape
    group = 8
    gshape = (group, cols)
    glane = lanes_of(gshape)
    gzero = jnp.zeros(gshape, jnp.float32)
    step1 = divisor(levels, STEP_S)
    for r in range(rows // group):
        rs = slice(r * group, (r + 1) * group)

        def downward(chunk, carry, rs=rs):
            state = [list(x) for x in carry]
            base = levels - step1 - chunk * step1
            for sub in range(step1):
                k = base + (step1 - 1 - sub)
                g, h, th = g_s[k, rs], h_s[k, rs], th_ref[k]
                y = s_s[k, rs]
                hw, he, hs, hn = hw_s[k, rs], he_s[k, rs], hs_s[k, rs], hn_s[k, rs]
                for m in range(members):
                    mass, ps, us, vs, ce, cw, cn, cs = state[m]
                    p, zu, zv = p1_ref[m, k, rs], zu_ref[m, k, rs], zv_ref[m, k, rs]
                    mass = mass + ((g * p + y * w1_ref[m, k, rs]) + h * (zu + zv))
                    ps = ps + th * p
                    us = us + th * zu
                    vs = vs + th * zv
                    ce = ce + hw * zu
                    cw = cw + he * p
                    cn = cn + hs * zv
                    cs = cs + hn * p
                    state[m] = [mass, ps, us, vs, ce, cw, cn, cs]
            return tuple(tuple(x) for x in state)

        out = lax.fori_loop(0, levels // step1, downward, ((gzero,) * 8,) * members)
        for m in range(members):
            mass, ps, us, vs, ce, cw, cn, cs = out[m]
            sums_ref[m, 0, rs] = mass - east_roll(ce) + west_roll(cw)
            sums_ref[m, 1, rs] = us + jnp.where(glane == 0, 0.0, HORIZ * west_roll(ps))
            sums_ref[m, 2, rs] = vs
            keep_s[m, 0, rs] = ps
            keep_s[m, 1, rs] = cn
            keep_s[m, 2, rs] = cs
    row = rows_of((rows, cols))
    for m in range(members):
        ps, cn, cs = keep_s[m, 0], keep_s[m, 1], keep_s[m, 2]
        sums_ref[m, 0] = sums_ref[m, 0] - north_roll(cn) + south_roll(cs)
        sums_ref[m, 2] = sums_ref[m, 2] + jnp.where(row == 0, 0.0, HORIZ * south_roll(ps))


def edge_kernel(sums_ref, far_ref, near_ref, from_rows, hcols_ref, hrows_ref, hth_ref, *rest):
    outs, total_s = rest[:-1], rest[-1]
    from_west, from_east = sides(far_ref, near_ref)
    members, _, rows, cols = sums_ref.shape
    levels = hrows_ref.shape[1]
    height = rows // len(outs)
    mine = lax.axis_index("mem")
    lane = lanes_of((rows, cols))
    row = rows_of((rows, cols))
    even = lane % 2 == 0
    used = lane < 2 * levels
    hth = jnp.concatenate([hth_ref[...]] * (rows // 8), axis=0)
    for m in range(members):
        west = west_roll(from_west[m])
        products = jnp.where(used, hcols_ref[...] * jnp.where(even, east_roll(from_east[m]), west), 0.0)
        at_east = jnp.sum(jnp.where(even, products, 0.0), axis=1, keepdims=True)
        at_west = jnp.sum(jnp.where(even, 0.0, products), axis=1, keepdims=True)
        u_west = jnp.sum(hth * west, axis=1, keepdims=True)
        at_south = jnp.sum(hrows_ref[0] * from_rows[0, m], axis=0, keepdims=True)
        at_north = jnp.sum(hrows_ref[1] * from_rows[1, m], axis=0, keepdims=True)
        v_south = jnp.sum(hrows_ref[2] * from_rows[0, m], axis=0, keepdims=True)
        mass = sums_ref[m, 0] + jnp.where(lane == 0, at_west, 0.0) + jnp.where(lane == cols - 1, at_east, 0.0)
        mass = mass + jnp.where(row == 0, at_south, 0.0) - jnp.where(row == rows - 1, at_north, 0.0)
        total_s[m, 0] = mass
        total_s[m, 1] = sums_ref[m, 1] + jnp.where(lane == 0, u_west, 0.0)
        total_s[m, 2] = sums_ref[m, 2] + jnp.where(row == 0, v_south, 0.0)
    for d, out_ref in enumerate(outs):
        start = pl.multiple_of((mine ^ d) * height, height)
        out_ref[...] = total_s[:, :, pl.ds(start, height), :]


def stats_kernel(*refs):
    ins, out_ref = refs[:-1], refs[-1]
    members, fields = ins[0].shape[:2]
    count = len(ins) * members
    for f in range(fields):
        values = [ref[m, f] for ref in ins for m in range(members)]
        mean = functools.reduce(jnp.add, values) / count
        square = functools.reduce(jnp.add, [(v - mean) * (v - mean) for v in values]) / (count - 1)
        out_ref[f] = mean
        out_ref[fields + f] = square


def select_kernel(width, masks_ref, *refs):
    tiles, outs = refs[:-width], refs[-width:]
    for d, out_ref in enumerate(outs):
        for f in range(out_ref.shape[0]):
            value = tiles[0][f]
            for j in range(1, len(tiles)):
                value = jnp.where(masks_ref[j * width + d] > 0.5, tiles[j][f], value)
            out_ref[f] = value


def pick_kernel(masks_ref, *refs):
    ins, out_ref = refs[:-1], refs[-1]
    width = len(ins)
    base = masks_ref.shape[0] - width
    for f in range(ins[0].shape[0]):
        value = ins[0][f]
        for d in range(1, width):
            value = jnp.where(masks_ref[base + d] > 0.5, ins[d][f], value)
        out_ref[0, 0, f] = value


def call(kernel, outs, in_specs, scratch=(), limit=16):
    return pl.pallas_call(
        kernel,
        out_shape=[jax.ShapeDtypeStruct(s, jnp.float32) for s in outs],
        in_specs=in_specs,
        out_specs=[VMEM] * len(outs),
        scratch_shapes=list(scratch),
        compiler_params=pltpu.CompilerParams(vmem_limit_bytes=limit * 1024 * 1024),
    )


def permuted(block, axis, source):
    count = lax.axis_size(axis)
    return lax.ppermute(block, axis, [(source(i) % count, i) for i in range(count)])


def exchange(columns, edge_rows):
    far = permuted(columns, "tx", lambda i: i + 1 if i % 2 else i - 1)
    near = permuted(columns, "tx", lambda i: i ^ 1)
    if lax.axis_size("ty") <= 2:
        both = permuted(edge_rows, "ty", lambda i: i - 1)
    else:
        south = permuted(edge_rows[0], "ty", lambda i: i - 1)
        north = permuted(edge_rows[1], "ty", lambda i: i + 1)
        both = jnp.stack([south, north])
    return far, near, both


def steps(pressure, east_wind, north_wind, vertical_wind, sound_squared, thickness, owner_map):
    members, levels, rows, cols = pressure.shape
    ranks, height_count, width = (lax.axis_size(a) for a in ("mem", "ty", "tx"))
    height = rows // ranks
    plane = (members, rows, cols)
    many = (members, levels, rows, cols)
    field = (levels, rows, cols)
    lines = (2, members, levels, cols)
    part = (6, height, cols)
    pressure, east_wind, north_wind, vertical_wind = (
        pltpu.with_memory_space_constraint(x, pltpu.HBM)
        for x in (pressure, east_wind, north_wind, vertical_wind)
    )
    columns, edge_rows, p0, u0 = call(
        pack_kernel,
        [plane, lines, many, many],
        [HBM] * 3,
        [
            pltpu.VMEM((members, levels, 8, cols), jnp.float32),
            pltpu.SemaphoreType.DMA((members, 3)),
        ],
        limit=PACK_LIMIT,
    )(pressure, east_wind, north_wind)
    far, near, both = exchange(columns, edge_rows)
    hcols, hrows, hth, masks, e, inv, *weights, part0, u0, v0, w0 = call(
        prepare_kernel,
        [
            (rows, cols),
            (3, levels, cols),
            (8, cols),
            (height_count * width + width, 8, cols),
            *[field] * 9,
            *[many] * 3,
            vertical_wind.shape,
        ],
        [VMEM, VMEM, VMEM, HBM, HBM, SMEM, SMEM],
        [pltpu.SemaphoreType.DMA((2, members))],
        limit=PREP_LIMIT,
    )(sound_squared, p0, u0, north_wind, vertical_wind, thickness, owner_map)
    columns, edge_rows, p1, zu, zv, w1 = call(
        solve_kernel, [plane, lines, *[many] * 4], [VMEM] * 10
    )(sound_squared, part0, u0, v0, w0, e, inv, far, near, both)
    far, near, both = exchange(columns, edge_rows)
    (sums,) = call(
        sum_kernel,
        [(members, 3, rows, cols)],
        [VMEM] * 4 + [SMEM] + [VMEM] * 7,
        [pltpu.VMEM((members, 3, rows, cols), jnp.float32)],
    )(p1, zu, zv, w1, thickness, *weights)
    quarters = call(
        edge_kernel,
        [(members, 3, height, cols)] * ranks,
        [VMEM] * 7,
        [pltpu.VMEM((members, 3, rows, cols), jnp.float32)],
    )(sums, far, near, both, hcols, hrows, hth)
    quarters = [
        permuted(x, "mem", lambda i, d=d: i ^ d) if d else x for d, x in enumerate(quarters)
    ]
    (stats,) = call(stats_kernel, [part], [VMEM] * ranks)(*quarters)
    tiles = [
        permuted(stats, "ty", lambda i, j=j: i ^ j) if j else stats
        for j in range(height_count)
    ]
    chosen = call(
        functools.partial(select_kernel, width), [part] * width, [VMEM] * (1 + height_count)
    )(masks, *tiles)
    routed = [permuted(x, "tx", lambda i, d=d: i ^ d) if d else x for d, x in enumerate(chosen)]
    (result,) = call(pick_kernel, [(1, 1) + part], [VMEM] * (1 + width))(masks, *routed)
    return result


def solution(mesh):
    placed = (
        P("mem", None, "ty", "tx"),
        P("mem", None, "ty", "tx"),
        P("mem", None, "ty", "tx"),
        P("mem", None, "ty", "tx"),
        P(None, "ty", "tx"),
        P(),
        P(),
    )
    return jax.shard_map(
        steps,
        mesh=mesh,
        in_specs=placed,
        out_specs=P("ty", "tx", None, "mem", None),
        check_vma=False,
    )
```

```python
import functools

import jax
import jax.numpy as jnp
from jax import lax
from jax.experimental import pallas as pl
from jax.experimental.pallas import tpu as pltpu
from jax.sharding import PartitionSpec as P


HORIZ = 0.35
VERT = 1.5
STEP_A = 8
STEP_P = 25
STEP_B = 25
STEP_D = 25
STEP_S = 25
PACK_LIMIT = 16
PREP_LIMIT = 24

VMEM = pl.BlockSpec(memory_space=pltpu.VMEM)
SMEM = pl.BlockSpec(memory_space=pltpu.SMEM)
HBM = pl.BlockSpec(memory_space=pltpu.HBM)


def divisor(count, most):
    return max(d for d in range(1, most + 1) if count % d == 0)


def lanes_of(shape):
    return lax.broadcasted_iota(jnp.int32, shape, len(shape) - 1)


def rows_of(shape):
    return lax.broadcasted_iota(jnp.int32, shape, len(shape) - 2)


def west_roll(x):
    return pltpu.roll(x, 1, 1)


def east_roll(x):
    return pltpu.roll(x, x.shape[1] - 1, 1)


def south_roll(x):
    return pltpu.roll(x, 1, 0)


def north_roll(x):
    return pltpu.roll(x, x.shape[0] - 1, 0)


def outgoing(packed, far_ref, near_ref):
    odd = lax.axis_index("tx") % 2 == 1
    even = lanes_of(packed[0].shape) % 2 == 0
    eastward = jnp.where(even, packed[0], west_roll(packed[1]))
    westward = jnp.where(even, east_roll(packed[0]), packed[1])
    far_ref[...] = jnp.where(odd, eastward, westward)
    near_ref[...] = jnp.where(odd, westward, eastward)


def incoming(far_ref, near_ref):
    odd = lax.axis_index("tx") % 2 == 1
    far, near = far_ref[...], near_ref[...]
    even = lanes_of(far.shape) % 2 == 0
    west, east = jnp.where(odd, near, far), jnp.where(odd, far, near)
    return [jnp.where(even, east, west_roll(west)), jnp.where(even, east_roll(east), west)]


def pack_kernel(p_hbm, u_hbm, v_hbm, far_ref, near_ref, rows_ref, p_ref, u_ref, v_s, sems):
    members, levels, rows, cols = p_ref.shape
    planes = []
    copies = []
    for m in range(members):
        pair = [
            pltpu.make_async_copy(p_hbm.at[m], p_ref.at[m], sems.at[m, 0]),
            pltpu.make_async_copy(u_hbm.at[m], u_ref.at[m], sems.at[m, 1]),
            pltpu.make_async_copy(v_hbm.at[m, :, 0:8], v_s.at[m], sems.at[m, 2]),
        ]
        for copy in pair:
            copy.start()
        copies.append(pair)
    lane = lanes_of((rows, cols))
    for m in range(members):
        for copy in copies[m]:
            copy.wait()
        packed = jnp.zeros((rows, cols), jnp.float32)
        for k in range(levels):
            p = p_ref[m, k]
            z = u_ref[m, k] - HORIZ * p
            edge = pltpu.roll(jnp.where(lane == cols - 1, p, z), 2 * k + 1, 1)
            packed = jnp.where(lane >= 2 * k, edge, packed)
            rows_ref[0, m, k : k + 1, :] = p[rows - 1 : rows, :]
            rows_ref[1, m, k : k + 1, :] = v_s[m, k, 0:1, :] - HORIZ * p[0:1, :]
        planes.append(packed)
    outgoing(planes, far_ref, near_ref)


def prepare_kernel(
    c_ref, p_ref, u0_ref, v_hbm, w_hbm, th_ref, owner_ref,
    hcols_ref, hrows_ref, hth_ref, masks_ref,
    e_s, inv_s, s_s, g_s, h_s, hw_s, he_s, hs_s, hn_s, part_ref, u_ref, v_ref, w_ref, sems,
):
    members, levels, rows, cols = part_ref.shape
    copies = [
        pltpu.make_async_copy(source.at[m], target.at[m], sems.at[i, m])
        for i, (source, target) in enumerate([(v_hbm, v_ref), (w_hbm, w_ref)])
        for m in range(members)
    ]
    for copy in copies:
        copy.start()
    inner = levels - 1
    shape = (rows, cols)
    lane = lanes_of(shape)
    row = rows_of(shape)
    first_lane, last_lane = lane == 0, lane == cols - 1
    first_row, last_row = row == 0, row == rows - 1
    zero = jnp.zeros(shape, jnp.float32)
    vsq = VERT * VERT

    height, width = lax.axis_size("ty"), lax.axis_size("tx")
    my_row, my_column = lax.axis_index("ty"), lax.axis_index("tx")
    mask = (8, cols)
    for j in range(height):
        for d in range(width):
            here = owner_ref[(my_row ^ j) * width + my_column] == my_row * width + (my_column ^ d)
            masks_ref[j * width + d] = jnp.full(mask, jnp.where(here, 1.0, 0.0), jnp.float32)
    for d in range(width):
        here = jnp.float32(0.0)
        for j in range(height):
            mine = owner_ref[j * width + (my_column ^ d)] == my_row * width + my_column
            here = jnp.where(mine, 1.0, here)
        masks_ref[height * width + d] = jnp.full(mask, here, jnp.float32)

    for ref in (e_s, inv_s, s_s):
        ref[0] = zero

    step = divisor(inner, STEP_A)

    def factor(chunk, carry):
        e_prev, s_prev, c_here = carry
        for sub in range(step):
            i = chunk * step + sub
            c_next = c_ref[i + 1]
            b_next = vsq * c_next
            pivot = (1.0 + b_next) + (vsq * c_here) * (1.0 - e_prev)
            inv = 1.0 / pivot
            s_prev = VERT * (th_ref[i + 1] * c_next - th_ref[i] * c_here) + e_prev * s_prev
            e_prev = b_next * inv
            e_s[i + 1] = e_prev
            inv_s[i + 1] = inv
            s_s[i + 1] = s_prev * inv
            c_here = c_next
        return e_prev, s_prev, c_here

    lax.fori_loop(0, inner // step, factor, (zero, zero, c_ref[0]))

    def weights(k, y_above, y_here):
        g = th_ref[k] + VERT * (y_above - y_here)
        h = g * (HORIZ * c_ref[k])
        g_s[k] = g - (2 * HORIZ) * h
        h_s[k] = h
        h35 = HORIZ * h
        hw_s[k] = jnp.where(first_lane, 0.0, west_roll(h))
        he_s[k] = jnp.where(last_lane, 0.0, east_roll(h35))
        hs_s[k] = jnp.where(first_row, 0.0, south_roll(h))
        hn_s[k] = jnp.where(last_row, 0.0, north_roll(h35))
        hrows_ref[0, pl.ds(k, 1), :] = h35[0:1, :]
        hrows_ref[1, pl.ds(k, 1), :] = h[rows - 1 : rows, :]
        hrows_ref[2, pl.ds(k, 1), :] = jnp.full((1, cols), HORIZ * th_ref[k], jnp.float32)
        return jnp.where(last_lane, -h, h35)

    def adjoint(chunk, carry):
        y_above, packed = carry
        packed = pltpu.roll(packed, 2 * step, 1)
        for sub in range(step):
            i = inner - 1 - (chunk * step + sub)
            y_here = s_s[i + 1] + e_s[i + 1] * y_above
            s_s[i + 1] = y_here
            edge = weights(i + 1, y_above, y_here)
            place = 2 * (step - 1 - sub)
            packed = jnp.where(lane < place + 2, pltpu.roll(edge, place + 1, 1), packed)
            y_above = y_here
        return y_above, packed

    y_low, packed = lax.fori_loop(0, inner // step, adjoint, (zero, zero))
    edge = weights(0, y_low, zero)
    hcols_ref[...] = jnp.where(lane < 2, pltpu.roll(edge, 1, 1), pltpu.roll(packed, 2, 1))
    hth = jnp.zeros(mask, jnp.float32)
    for k in range(levels):
        hth = jnp.where(lanes_of(mask) == 2 * k + 1, HORIZ * th_ref[k], hth)
    hth_ref[...] = hth

    for copy in copies[:members]:
        copy.wait()
    step1 = divisor(levels, STEP_P)

    group = 8
    slices = [slice(at, at + group) for at in range(0, rows, group)]
    glane, grow = lanes_of((group, cols)), rows_of((group, cols))
    west_edge, east_edge = glane == 0, glane == cols - 1

    def southern(x):
        x = [pltpu.roll(v, 1, 0) for v in x]
        return [jnp.where(grow == 0, x[i - 1] if i else 0.0, v) for i, v in enumerate(x)]

    def northern(x):
        x = [pltpu.roll(v, group - 1, 0) for v in x]
        after = x[1:] + [0.0]
        return [jnp.where(grow == group - 1, after[i], v) for i, v in enumerate(x)]

    def first_winds(chunk, carry):
        for sub in range(step1):
            k = chunk * step1 + sub
            for m in range(members):
                q, zv = [], []
                for rs in slices:
                    q.append(HORIZ * p_ref[m, k, rs])
                    zv.append(v_ref[m, k, rs] - q[-1])
                q_south, zv_north = southern(q), northern(zv)
                for i, rs in enumerate(slices):
                    zu = u0_ref[m, k, rs] - q[i]
                    u1 = zu + jnp.where(west_edge, 0.0, west_roll(q[i]))
                    v1 = zv[i] + q_south[i]
                    u_ref[m, k, rs] = u1
                    v_ref[m, k, rs] = v1
                    zu_east = jnp.where(east_edge, 0.0, east_roll(zu))
                    div = ((zu_east + q[i]) - u1) + ((zv_north[i] + q[i]) - v1)
                    part_ref[m, k, rs] = p_ref[m, k, rs] - (HORIZ * c_ref[k, rs]) * div
        return carry

    lax.fori_loop(0, levels // step1, first_winds, 0)
    for copy in copies[members:]:
        copy.wait()


def solve_kernel(
    c_ref, part_ref, u_ref, v_ref, w_ref, e_s, inv_s, far_ref, near_ref, from_rows,
    far_out, near_out, rows_ref, p1_ref, zu_ref, zv_ref, w1_ref,
):
    members, levels, rows, cols = part_ref.shape
    group = 8
    groups = rows // group
    gshape = (group, cols)
    slices = [slice(g * group, (g + 1) * group) for g in range(groups)]
    lane, row = lanes_of(gshape), rows_of(gshape)
    zero = jnp.zeros(gshape, jnp.float32)
    at_first = jnp.where(lane == 0, 1.0, 0.0)
    signed = jnp.where(lane == cols - 1, -1.0, at_first)
    even = lane % 2 == 0
    halo = []
    for mixed in incoming(far_ref, near_ref):
        for rs in slices:
            halo.append(east_roll(jnp.where(even, mixed[rs], HORIZ * mixed[rs])))
    step1 = divisor(levels, STEP_B)

    def upward(chunk, carry):
        part_prev, v_prev, halo = (list(x) for x in carry)
        for sub in range(step1):
            k = chunk * step1 + sub
            below = jnp.maximum(k - 1, 0)
            for g, rs in enumerate(slices):
                c35 = HORIZ * c_ref[k, rs]
                e = e_s[below, rs]
                for m in range(members):
                    at = m * groups + g
                    edge = halo[at] if sub == 0 else pltpu.roll(halo[at], cols - 2 * sub, 1)
                    zu_ref[m, k, rs] = u_ref[m, k, rs] + edge * at_first
                    delta = edge * signed
                    if g == 0:
                        delta = delta + jnp.where(row == 0, HORIZ * from_rows[0, m, pl.ds(k, 1), :], 0.0)
                    if g == groups - 1:
                        delta = delta - jnp.where(row == group - 1, from_rows[1, m, pl.ds(k, 1), :], 0.0)
                    part = part_ref[m, k, rs] + c35 * delta
                    p1_ref[m, k, rs] = part
                    rhs = w_ref[m, below, rs] - VERT * (part - part_prev[at])
                    v_new = rhs + e * v_prev[at]
                    w1_ref[m, k, rs] = v_new
                    v_prev[at] = v_new
                    part_prev[at] = part
        halo = [pltpu.roll(x, cols - 2 * step1, 1) for x in halo]
        return tuple(part_prev), tuple(v_prev), tuple(halo)

    zeros = (zero,) * (members * groups)
    lax.fori_loop(0, levels // step1, upward, (zeros, zeros, tuple(halo)))

    last = lane == cols - 1

    def downward(chunk, carry):
        ws, packs = list(carry[0]), list(carry[1])
        base = levels - step2 - chunk * step2
        for sub in range(step2):
            place = 2 * (step2 - 1 - sub)
            k = base + (step2 - 1 - sub)
            for g, rs in enumerate(slices):
                inv, e = inv_s[k, rs], e_s[k, rs]
                c15 = VERT * c_ref[k, rs]
                for m in range(members):
                    at = m * groups + g
                    w = ws[at]
                    w_low = w1_ref[m, k, rs] * inv + e * w
                    w1_ref[m, k, rs] = w_low
                    p = p1_ref[m, k, rs] - c15 * (w - w_low)
                    p1_ref[m, k, rs] = p
                    q = HORIZ * p
                    zu = zu_ref[m, k, rs] - q
                    zu_ref[m, k, rs] = zu
                    v1 = v_ref[m, k, rs]
                    if g == 0:
                        v1 = v1 + jnp.where(row == 0, HORIZ * from_rows[0, m, pl.ds(k, 1), :], 0.0)
                    zv = v1 - q
                    zv_ref[m, k, rs] = zv
                    edge = pltpu.roll(jnp.where(last, p, zu), place + 1, 1)
                    if sub == 0:
                        packs[at] = pltpu.roll(packs[at], 2 * step2, 1)
                    packs[at] = jnp.where(lane < place + 2, edge, packs[at])
                    if g == groups - 1:
                        rows_ref[0, m, pl.ds(k, 1), :] = p[group - 1 : group, :]
                    if g == 0:
                        rows_ref[1, m, pl.ds(k, 1), :] = zv[0:1, :]
                    ws[at] = w_low
        return tuple(ws), tuple(packs)

    step2 = divisor(levels, STEP_D)
    _, packs = lax.fori_loop(0, levels // step2, downward, (zeros, zeros))
    planes = [
        jnp.concatenate(packs[m * groups : (m + 1) * groups], axis=0) for m in range(members)
    ]
    outgoing(planes, far_out, near_out)


def sum_kernel(
    p1_ref, zu_ref, zv_ref, w1_ref, th_ref, s_s, g_s, h_s, hw_s, he_s, hs_s, hn_s, sums_ref, keep_s
):
    members, levels, rows, cols = p1_ref.shape
    group = 8
    gshape = (group, cols)
    glane = lanes_of(gshape)
    gzero = jnp.zeros(gshape, jnp.float32)
    step1 = divisor(levels, STEP_S)
    for r in range(rows // group):
        rs = slice(r * group, (r + 1) * group)

        def downward(chunk, carry, rs=rs):
            state = [list(x) for x in carry]
            base = levels - step1 - chunk * step1
            for sub in range(step1):
                k = base + (step1 - 1 - sub)
                g, h, th = g_s[k, rs], h_s[k, rs], th_ref[k]
                y = s_s[k, rs]
                hw, he, hs, hn = hw_s[k, rs], he_s[k, rs], hs_s[k, rs], hn_s[k, rs]
                for m in range(members):
                    mass, ps, us, vs, ce, cw, cn, cs = state[m]
                    p, zu, zv = p1_ref[m, k, rs], zu_ref[m, k, rs], zv_ref[m, k, rs]
                    mass = mass + ((g * p + y * w1_ref[m, k, rs]) + h * (zu + zv))
                    ps = ps + th * p
                    us = us + th * zu
                    vs = vs + th * zv
                    ce = ce + hw * zu
                    cw = cw + he * p
                    cn = cn + hs * zv
                    cs = cs + hn * p
                    state[m] = [mass, ps, us, vs, ce, cw, cn, cs]
            return tuple(tuple(x) for x in state)

        out = lax.fori_loop(0, levels // step1, downward, ((gzero,) * 8,) * members)
        for m in range(members):
            mass, ps, us, vs, ce, cw, cn, cs = out[m]
            sums_ref[m, 0, rs] = mass - east_roll(ce) + west_roll(cw)
            sums_ref[m, 1, rs] = us + jnp.where(glane == 0, 0.0, HORIZ * west_roll(ps))
            sums_ref[m, 2, rs] = vs
            keep_s[m, 0, rs] = ps
            keep_s[m, 1, rs] = cn
            keep_s[m, 2, rs] = cs
    row = rows_of((rows, cols))
    for m in range(members):
        ps, cn, cs = keep_s[m, 0], keep_s[m, 1], keep_s[m, 2]
        sums_ref[m, 0] = sums_ref[m, 0] - north_roll(cn) + south_roll(cs)
        sums_ref[m, 2] = sums_ref[m, 2] + jnp.where(row == 0, 0.0, HORIZ * south_roll(ps))


def edge_kernel(sums_ref, far_ref, near_ref, from_rows, hcols_ref, hrows_ref, hth_ref, *rest):
    outs, total_s = rest[:-1], rest[-1]
    mixed = incoming(far_ref, near_ref)
    members, _, rows, cols = sums_ref.shape
    levels = hrows_ref.shape[1]
    height = rows // len(outs)
    mine = lax.axis_index("mem")
    lane = lanes_of((rows, cols))
    row = rows_of((rows, cols))
    even = lane % 2 == 0
    used = lane < 2 * levels
    hth = jnp.concatenate([hth_ref[...]] * (rows // 8), axis=0)
    for m in range(members):
        products = jnp.where(used, hcols_ref[...] * mixed[m], 0.0)
        at_east = jnp.sum(jnp.where(even, products, 0.0), axis=1, keepdims=True)
        at_west = jnp.sum(jnp.where(even, 0.0, products), axis=1, keepdims=True)
        u_west = jnp.sum(hth * mixed[m], axis=1, keepdims=True)
        at_south = jnp.sum(hrows_ref[0] * from_rows[0, m], axis=0, keepdims=True)
        at_north = jnp.sum(hrows_ref[1] * from_rows[1, m], axis=0, keepdims=True)
        v_south = jnp.sum(hrows_ref[2] * from_rows[0, m], axis=0, keepdims=True)
        mass = sums_ref[m, 0] + jnp.where(lane == 0, at_west, 0.0) + jnp.where(lane == cols - 1, at_east, 0.0)
        mass = mass + jnp.where(row == 0, at_south, 0.0) - jnp.where(row == rows - 1, at_north, 0.0)
        total_s[m, 0] = mass
        total_s[m, 1] = sums_ref[m, 1] + jnp.where(lane == 0, u_west, 0.0)
        total_s[m, 2] = sums_ref[m, 2] + jnp.where(row == 0, v_south, 0.0)
    for d, out_ref in enumerate(outs):
        start = pl.multiple_of((mine ^ d) * height, height)
        out_ref[...] = total_s[:, :, pl.ds(start, height), :]


def stats_kernel(*refs):
    ins, out_ref = refs[:-1], refs[-1]
    members, fields = ins[0].shape[:2]
    count = len(ins) * members
    for f in range(fields):
        values = [ref[m, f] for ref in ins for m in range(members)]
        mean = functools.reduce(jnp.add, values) / count
        square = functools.reduce(jnp.add, [(v - mean) * (v - mean) for v in values]) / (count - 1)
        out_ref[f] = mean
        out_ref[fields + f] = square


def select_kernel(width, masks_ref, *refs):
    tiles, outs = refs[:-width], refs[-width:]
    for d, out_ref in enumerate(outs):
        for f in range(out_ref.shape[0]):
            value = tiles[0][f]
            for j in range(1, len(tiles)):
                value = jnp.where(masks_ref[j * width + d] > 0.5, tiles[j][f], value)
            out_ref[f] = value


def pick_kernel(masks_ref, *refs):
    ins, out_ref = refs[:-1], refs[-1]
    width = len(ins)
    base = masks_ref.shape[0] - width
    for f in range(ins[0].shape[0]):
        value = ins[0][f]
        for d in range(1, width):
            value = jnp.where(masks_ref[base + d] > 0.5, ins[d][f], value)
        out_ref[0, 0, f] = value


def call(kernel, outs, in_specs, scratch=(), limit=16):
    return pl.pallas_call(
        kernel,
        out_shape=[jax.ShapeDtypeStruct(s, jnp.float32) for s in outs],
        in_specs=in_specs,
        out_specs=[VMEM] * len(outs),
        scratch_shapes=list(scratch),
        compiler_params=pltpu.CompilerParams(vmem_limit_bytes=limit * 1024 * 1024),
    )


def permuted(block, axis, source):
    count = lax.axis_size(axis)
    return lax.ppermute(block, axis, [(source(i) % count, i) for i in range(count)])


def exchange(far, near, edge_rows):
    far = permuted(far, "tx", lambda i: i + 1 if i % 2 else i - 1)
    near = permuted(near, "tx", lambda i: i ^ 1)
    if lax.axis_size("ty") <= 2:
        both = permuted(edge_rows, "ty", lambda i: i - 1)
    else:
        south = permuted(edge_rows[0], "ty", lambda i: i - 1)
        north = permuted(edge_rows[1], "ty", lambda i: i + 1)
        both = jnp.stack([south, north])
    return far, near, both


def steps(pressure, east_wind, north_wind, vertical_wind, sound_squared, thickness, owner_map):
    members, levels, rows, cols = pressure.shape
    ranks, height_count, width = (lax.axis_size(a) for a in ("mem", "ty", "tx"))
    height = rows // ranks
    plane = (rows, cols)
    many = (members, levels, rows, cols)
    field = (levels, rows, cols)
    lines = (2, members, levels, cols)
    part = (6, height, cols)
    pressure, east_wind, north_wind, vertical_wind = (
        pltpu.with_memory_space_constraint(x, pltpu.HBM)
        for x in (pressure, east_wind, north_wind, vertical_wind)
    )
    far, near, edge_rows, p0, u0 = call(
        pack_kernel,
        [plane, plane, lines, many, many],
        [HBM] * 3,
        [
            pltpu.VMEM((members, levels, 8, cols), jnp.float32),
            pltpu.SemaphoreType.DMA((members, 3)),
        ],
        limit=PACK_LIMIT,
    )(pressure, east_wind, north_wind)
    far, near, both = exchange(far, near, edge_rows)
    hcols, hrows, hth, masks, e, inv, *weights, part0, u0, v0, w0 = call(
        prepare_kernel,
        [
            (rows, cols),
            (3, levels, cols),
            (8, cols),
            (height_count * width + width, 8, cols),
            *[field] * 9,
            *[many] * 3,
            vertical_wind.shape,
        ],
        [VMEM, VMEM, VMEM, HBM, HBM, SMEM, SMEM],
        [pltpu.SemaphoreType.DMA((2, members))],
        limit=PREP_LIMIT,
    )(sound_squared, p0, u0, north_wind, vertical_wind, thickness, owner_map)
    far, near, edge_rows, p1, zu, zv, w1 = call(
        solve_kernel, [plane, plane, lines, *[many] * 4], [VMEM] * 10
    )(sound_squared, part0, u0, v0, w0, e, inv, far, near, both)
    far, near, both = exchange(far, near, edge_rows)
    (sums,) = call(
        sum_kernel,
        [(members, 3, rows, cols)],
        [VMEM] * 4 + [SMEM] + [VMEM] * 7,
        [pltpu.VMEM((members, 3, rows, cols), jnp.float32)],
    )(p1, zu, zv, w1, thickness, *weights)
    quarters = call(
        edge_kernel,
        [(members, 3, height, cols)] * ranks,
        [VMEM] * 7,
        [pltpu.VMEM((members, 3, rows, cols), jnp.float32)],
    )(sums, far, near, both, hcols, hrows, hth)
    quarters = [
        permuted(x, "mem", lambda i, d=d: i ^ d) if d else x for d, x in enumerate(quarters)
    ]
    (stats,) = call(stats_kernel, [part], [VMEM] * ranks)(*quarters)
    tiles = [
        permuted(stats, "ty", lambda i, j=j: i ^ j) if j else stats
        for j in range(height_count)
    ]
    chosen = call(
        functools.partial(select_kernel, width), [part] * width, [VMEM] * (1 + height_count)
    )(masks, *tiles)
    routed = [permuted(x, "tx", lambda i, d=d: i ^ d) if d else x for d, x in enumerate(chosen)]
    (result,) = call(pick_kernel, [(1, 1) + part], [VMEM] * (1 + width))(masks, *routed)
    return result


def solution(mesh):
    placed = (
        P("mem", None, "ty", "tx"),
        P("mem", None, "ty", "tx"),
        P("mem", None, "ty", "tx"),
        P("mem", None, "ty", "tx"),
        P(None, "ty", "tx"),
        P(),
        P(),
    )
    return jax.shard_map(
        steps,
        mesh=mesh,
        in_specs=placed,
        out_specs=P("ty", "tx", None, "mem", None),
        check_vma=False,
    )
```

```python
import functools

import jax
import jax.numpy as jnp
from jax import lax
from jax.experimental import pallas as pl
from jax.experimental.pallas import tpu as pltpu
from jax.sharding import PartitionSpec as P


HORIZ = 0.35
VERT = 1.5
STEP_A = 8
STEP_P = 25
STEP_B = 25
STEP_D = 25
STEP_S = 25
PACK_LIMIT = 16
PREP_LIMIT = 24

VMEM = pl.BlockSpec(memory_space=pltpu.VMEM)
SMEM = pl.BlockSpec(memory_space=pltpu.SMEM)
HBM = pl.BlockSpec(memory_space=pltpu.HBM)


def divisor(count, most):
    return max(d for d in range(1, most + 1) if count % d == 0)


def lanes_of(shape):
    return lax.broadcasted_iota(jnp.int32, shape, len(shape) - 1)


def rows_of(shape):
    return lax.broadcasted_iota(jnp.int32, shape, len(shape) - 2)


def west_roll(x):
    return pltpu.roll(x, 1, 1)


def east_roll(x):
    return pltpu.roll(x, x.shape[1] - 1, 1)


def south_roll(x):
    return pltpu.roll(x, 1, 0)


def north_roll(x):
    return pltpu.roll(x, x.shape[0] - 1, 0)


def outgoing(packed, far_ref, near_ref):
    odd = lax.axis_index("tx") % 2 == 1
    even = lanes_of(packed[0].shape) % 2 == 0
    eastward = jnp.where(even, packed[0], west_roll(packed[1]))
    westward = jnp.where(even, east_roll(packed[0]), packed[1])
    far_ref[...] = jnp.where(odd, eastward, westward)
    near_ref[...] = jnp.where(odd, westward, eastward)


def incoming(far_ref, near_ref):
    odd = lax.axis_index("tx") % 2 == 1
    far, near = far_ref[...], near_ref[...]
    even = lanes_of(far.shape) % 2 == 0
    west, east = jnp.where(odd, near, far), jnp.where(odd, far, near)
    return [jnp.where(even, east, west_roll(west)), jnp.where(even, east_roll(east), west)]


def pack_kernel(p_hbm, u_hbm, v_hbm, far_ref, near_ref, rows_ref, p_ref, u_ref, v_s, sems):
    members, levels, rows, cols = p_ref.shape
    planes = []
    copies = []
    for m in range(members):
        pair = [
            pltpu.make_async_copy(p_hbm.at[m], p_ref.at[m], sems.at[m, 0]),
            pltpu.make_async_copy(u_hbm.at[m], u_ref.at[m], sems.at[m, 1]),
            pltpu.make_async_copy(v_hbm.at[m, :, 0:8], v_s.at[m], sems.at[m, 2]),
        ]
        for copy in pair:
            copy.start()
        copies.append(pair)
    lane = lanes_of((rows, cols))
    for m in range(members):
        for copy in copies[m]:
            copy.wait()
        packed = jnp.zeros((rows, cols), jnp.float32)
        for k in range(levels):
            p = p_ref[m, k]
            z = u_ref[m, k] - HORIZ * p
            edge = pltpu.roll(jnp.where(lane == cols - 1, p, z), 2 * k + 1, 1)
            packed = jnp.where(lane >= 2 * k, edge, packed)
            rows_ref[0, m, k : k + 1, :] = p[rows - 1 : rows, :]
            rows_ref[1, m, k : k + 1, :] = v_s[m, k, 0:1, :] - HORIZ * p[0:1, :]
        planes.append(packed)
    outgoing(planes, far_ref, near_ref)


def prepare_kernel(
    c_ref, p_ref, u0_ref, v_hbm, w_hbm, th_ref, owner_ref,
    hcols_ref, hrows_ref, hth_ref, masks_ref,
    e_s, inv_s, s_s, g_s, h_s, hw_s, he_s, hs_s, hn_s, part_ref, u_ref, v_ref, w_ref, sems,
):
    members, levels, rows, cols = part_ref.shape
    copies = [
        pltpu.make_async_copy(source.at[m], target.at[m], sems.at[i, m])
        for i, (source, target) in enumerate([(v_hbm, v_ref), (w_hbm, w_ref)])
        for m in range(members)
    ]
    for copy in copies:
        copy.start()
    inner = levels - 1
    shape = (rows, cols)
    lane = lanes_of(shape)
    first_lane, last_lane = lane == 0, lane == cols - 1
    zero = jnp.zeros(shape, jnp.float32)
    vsq = VERT * VERT

    height, width = lax.axis_size("ty"), lax.axis_size("tx")
    my_row, my_column = lax.axis_index("ty"), lax.axis_index("tx")
    mask = (8, cols)
    for j in range(height):
        for d in range(width):
            here = owner_ref[(my_row ^ j) * width + my_column] == my_row * width + (my_column ^ d)
            masks_ref[j * width + d] = jnp.full(mask, jnp.where(here, 1.0, 0.0), jnp.float32)
    for d in range(width):
        here = jnp.float32(0.0)
        for j in range(height):
            mine = owner_ref[j * width + (my_column ^ d)] == my_row * width + my_column
            here = jnp.where(mine, 1.0, here)
        masks_ref[height * width + d] = jnp.full(mask, here, jnp.float32)

    for ref in (e_s, inv_s, s_s):
        ref[0] = zero

    step = divisor(inner, STEP_A)

    def factor(chunk, carry):
        e_prev, s_prev, c_here = carry
        for sub in range(step):
            i = chunk * step + sub
            c_next = c_ref[i + 1]
            b_next = vsq * c_next
            pivot = (1.0 + b_next) + (vsq * c_here) * (1.0 - e_prev)
            inv = 1.0 / pivot
            s_prev = VERT * (th_ref[i + 1] * c_next - th_ref[i] * c_here) + e_prev * s_prev
            e_prev = b_next * inv
            e_s[i + 1] = e_prev
            inv_s[i + 1] = inv
            s_s[i + 1] = s_prev * inv
            c_here = c_next
        return e_prev, s_prev, c_here

    lax.fori_loop(0, inner // step, factor, (zero, zero, c_ref[0]))

    group = 8
    slices = [slice(at, at + group) for at in range(0, rows, group)]
    glane, grow = lanes_of((group, cols)), rows_of((group, cols))
    west_edge, east_edge = glane == 0, glane == cols - 1

    def southern(x):
        x = [pltpu.roll(v, 1, 0) for v in x]
        return [jnp.where(grow == 0, x[i - 1] if i else 0.0, v) for i, v in enumerate(x)]

    def northern(x):
        x = [pltpu.roll(v, group - 1, 0) for v in x]
        after = x[1:] + [0.0]
        return [jnp.where(grow == group - 1, after[i], v) for i, v in enumerate(x)]

    def weights(k, y_above, y_here):
        g = th_ref[k] + VERT * (y_above - y_here)
        h = g * (HORIZ * c_ref[k])
        g_s[k] = g - (2 * HORIZ) * h
        h_s[k] = h
        h35 = HORIZ * h
        hw_s[k] = jnp.where(first_lane, 0.0, west_roll(h))
        he_s[k] = jnp.where(last_lane, 0.0, east_roll(h35))
        h_south = southern([h[rs] for rs in slices])
        h_north = northern([h35[rs] for rs in slices])
        for i, rs in enumerate(slices):
            hs_s[k, rs] = h_south[i]
            hn_s[k, rs] = h_north[i]
        hrows_ref[0, pl.ds(k, 1), :] = h35[0:1, :]
        hrows_ref[1, pl.ds(k, 1), :] = h[rows - 1 : rows, :]
        hrows_ref[2, pl.ds(k, 1), :] = jnp.full((1, cols), HORIZ * th_ref[k], jnp.float32)
        return jnp.where(last_lane, -h, h35)

    def adjoint(chunk, carry):
        y_above, packed = carry
        packed = pltpu.roll(packed, 2 * step, 1)
        for sub in range(step):
            i = inner - 1 - (chunk * step + sub)
            y_here = s_s[i + 1] + e_s[i + 1] * y_above
            s_s[i + 1] = y_here
            edge = weights(i + 1, y_above, y_here)
            place = 2 * (step - 1 - sub)
            packed = jnp.where(lane < place + 2, pltpu.roll(edge, place + 1, 1), packed)
            y_above = y_here
        return y_above, packed

    y_low, packed = lax.fori_loop(0, inner // step, adjoint, (zero, zero))
    edge = weights(0, y_low, zero)
    hcols_ref[...] = jnp.where(lane < 2, pltpu.roll(edge, 1, 1), pltpu.roll(packed, 2, 1))
    hth = jnp.zeros(mask, jnp.float32)
    for k in range(levels):
        hth = jnp.where(lanes_of(mask) == 2 * k + 1, HORIZ * th_ref[k], hth)
    hth_ref[...] = hth

    for copy in copies[:members]:
        copy.wait()
    step1 = divisor(levels, STEP_P)

    def first_winds(chunk, carry):
        for sub in range(step1):
            k = chunk * step1 + sub
            for m in range(members):
                q, zv = [], []
                for rs in slices:
                    q.append(HORIZ * p_ref[m, k, rs])
                    zv.append(v_ref[m, k, rs] - q[-1])
                q_south, zv_north = southern(q), northern(zv)
                for i, rs in enumerate(slices):
                    zu = u0_ref[m, k, rs] - q[i]
                    u1 = zu + jnp.where(west_edge, 0.0, west_roll(q[i]))
                    v1 = zv[i] + q_south[i]
                    u_ref[m, k, rs] = u1
                    v_ref[m, k, rs] = v1
                    zu_east = jnp.where(east_edge, 0.0, east_roll(zu))
                    div = ((zu_east + q[i]) - u1) + ((zv_north[i] + q[i]) - v1)
                    part_ref[m, k, rs] = p_ref[m, k, rs] - (HORIZ * c_ref[k, rs]) * div
        return carry

    lax.fori_loop(0, levels // step1, first_winds, 0)
    for copy in copies[members:]:
        copy.wait()


def solve_kernel(
    c_ref, part_ref, u_ref, v_ref, w_ref, e_s, inv_s, far_ref, near_ref, from_rows,
    far_out, near_out, rows_ref, p1_ref, zu_ref, zv_ref, w1_ref,
):
    members, levels, rows, cols = part_ref.shape
    group = 8
    groups = rows // group
    gshape = (group, cols)
    slices = [slice(g * group, (g + 1) * group) for g in range(groups)]
    lane, row = lanes_of(gshape), rows_of(gshape)
    zero = jnp.zeros(gshape, jnp.float32)
    at_first = jnp.where(lane == 0, 1.0, 0.0)
    signed = jnp.where(lane == cols - 1, -1.0, at_first)
    even = lane % 2 == 0
    halo = []
    for mixed in incoming(far_ref, near_ref):
        for rs in slices:
            halo.append(east_roll(jnp.where(even, mixed[rs], HORIZ * mixed[rs])))
    step1 = divisor(levels, STEP_B)

    def upward(chunk, carry):
        part_prev, v_prev, halo = (list(x) for x in carry)
        for sub in range(step1):
            k = chunk * step1 + sub
            below = jnp.maximum(k - 1, 0)
            for g, rs in enumerate(slices):
                c35 = HORIZ * c_ref[k, rs]
                e = e_s[below, rs]
                for m in range(members):
                    at = m * groups + g
                    edge = halo[at] if sub == 0 else pltpu.roll(halo[at], cols - 2 * sub, 1)
                    zu_ref[m, k, rs] = u_ref[m, k, rs] + edge * at_first
                    delta = edge * signed
                    if g == 0:
                        delta = delta + jnp.where(row == 0, HORIZ * from_rows[0, m, pl.ds(k, 1), :], 0.0)
                    if g == groups - 1:
                        delta = delta - jnp.where(row == group - 1, from_rows[1, m, pl.ds(k, 1), :], 0.0)
                    part = part_ref[m, k, rs] + c35 * delta
                    p1_ref[m, k, rs] = part
                    rhs = w_ref[m, below, rs] - VERT * (part - part_prev[at])
                    v_new = rhs + e * v_prev[at]
                    w1_ref[m, k, rs] = v_new
                    v_prev[at] = v_new
                    part_prev[at] = part
        halo = [pltpu.roll(x, cols - 2 * step1, 1) for x in halo]
        return tuple(part_prev), tuple(v_prev), tuple(halo)

    zeros = (zero,) * (members * groups)
    lax.fori_loop(0, levels // step1, upward, (zeros, zeros, tuple(halo)))

    last = lane == cols - 1

    def downward(chunk, carry):
        ws, packs = list(carry[0]), list(carry[1])
        base = levels - step2 - chunk * step2
        for sub in range(step2):
            place = 2 * (step2 - 1 - sub)
            k = base + (step2 - 1 - sub)
            for g, rs in enumerate(slices):
                inv, e = inv_s[k, rs], e_s[k, rs]
                c15 = VERT * c_ref[k, rs]
                for m in range(members):
                    at = m * groups + g
                    w = ws[at]
                    w_low = w1_ref[m, k, rs] * inv + e * w
                    w1_ref[m, k, rs] = w_low
                    p = p1_ref[m, k, rs] - c15 * (w - w_low)
                    p1_ref[m, k, rs] = p
                    q = HORIZ * p
                    zu = zu_ref[m, k, rs] - q
                    zu_ref[m, k, rs] = zu
                    v1 = v_ref[m, k, rs]
                    if g == 0:
                        v1 = v1 + jnp.where(row == 0, HORIZ * from_rows[0, m, pl.ds(k, 1), :], 0.0)
                    zv = v1 - q
                    zv_ref[m, k, rs] = zv
                    edge = pltpu.roll(jnp.where(last, p, zu), place + 1, 1)
                    if sub == 0:
                        packs[at] = pltpu.roll(packs[at], 2 * step2, 1)
                    packs[at] = jnp.where(lane < place + 2, edge, packs[at])
                    if g == groups - 1:
                        rows_ref[0, m, pl.ds(k, 1), :] = p[group - 1 : group, :]
                    if g == 0:
                        rows_ref[1, m, pl.ds(k, 1), :] = zv[0:1, :]
                    ws[at] = w_low
        return tuple(ws), tuple(packs)

    step2 = divisor(levels, STEP_D)
    _, packs = lax.fori_loop(0, levels // step2, downward, (zeros, zeros))
    planes = [
        jnp.concatenate(packs[m * groups : (m + 1) * groups], axis=0) for m in range(members)
    ]
    outgoing(planes, far_out, near_out)


def sum_kernel(
    p1_ref, zu_ref, zv_ref, w1_ref, th_ref, s_s, g_s, h_s, hw_s, he_s, hs_s, hn_s, sums_ref, keep_s
):
    members, levels, rows, cols = p1_ref.shape
    group = 8
    gshape = (group, cols)
    glane = lanes_of(gshape)
    gzero = jnp.zeros(gshape, jnp.float32)
    step1 = divisor(levels, STEP_S)
    for r in range(rows // group):
        rs = slice(r * group, (r + 1) * group)

        def downward(chunk, carry, rs=rs):
            state = [list(x) for x in carry]
            base = levels - step1 - chunk * step1
            for sub in range(step1):
                k = base + (step1 - 1 - sub)
                g, h, th = g_s[k, rs], h_s[k, rs], th_ref[k]
                y = s_s[k, rs]
                hw, he, hs, hn = hw_s[k, rs], he_s[k, rs], hs_s[k, rs], hn_s[k, rs]
                for m in range(members):
                    mass, ps, us, vs, ce, cw, cn, cs = state[m]
                    p, zu, zv = p1_ref[m, k, rs], zu_ref[m, k, rs], zv_ref[m, k, rs]
                    mass = mass + ((g * p + y * w1_ref[m, k, rs]) + h * (zu + zv))
                    ps = ps + th * p
                    us = us + th * zu
                    vs = vs + th * zv
                    ce = ce + hw * zu
                    cw = cw + he * p
                    cn = cn + hs * zv
                    cs = cs + hn * p
                    state[m] = [mass, ps, us, vs, ce, cw, cn, cs]
            return tuple(tuple(x) for x in state)

        out = lax.fori_loop(0, levels // step1, downward, ((gzero,) * 8,) * members)
        for m in range(members):
            mass, ps, us, vs, ce, cw, cn, cs = out[m]
            sums_ref[m, 0, rs] = mass - east_roll(ce) + west_roll(cw)
            sums_ref[m, 1, rs] = us + jnp.where(glane == 0, 0.0, HORIZ * west_roll(ps))
            sums_ref[m, 2, rs] = vs
            keep_s[m, 0, rs] = ps
            keep_s[m, 1, rs] = cn
            keep_s[m, 2, rs] = cs
    row = rows_of((rows, cols))
    for m in range(members):
        ps, cn, cs = keep_s[m, 0], keep_s[m, 1], keep_s[m, 2]
        sums_ref[m, 0] = sums_ref[m, 0] - north_roll(cn) + south_roll(cs)
        sums_ref[m, 2] = sums_ref[m, 2] + jnp.where(row == 0, 0.0, HORIZ * south_roll(ps))


def edge_kernel(sums_ref, far_ref, near_ref, from_rows, hcols_ref, hrows_ref, hth_ref, *rest):
    outs, total_s = rest[:-1], rest[-1]
    mixed = incoming(far_ref, near_ref)
    members, _, rows, cols = sums_ref.shape
    levels = hrows_ref.shape[1]
    height = rows // len(outs)
    mine = lax.axis_index("mem")
    lane = lanes_of((rows, cols))
    row = rows_of((rows, cols))
    even = lane % 2 == 0
    used = lane < 2 * levels
    hth = jnp.concatenate([hth_ref[...]] * (rows // 8), axis=0)
    for m in range(members):
        products = jnp.where(used, hcols_ref[...] * mixed[m], 0.0)
        at_east = jnp.sum(jnp.where(even, products, 0.0), axis=1, keepdims=True)
        at_west = jnp.sum(jnp.where(even, 0.0, products), axis=1, keepdims=True)
        u_west = jnp.sum(hth * mixed[m], axis=1, keepdims=True)
        at_south = jnp.sum(hrows_ref[0] * from_rows[0, m], axis=0, keepdims=True)
        at_north = jnp.sum(hrows_ref[1] * from_rows[1, m], axis=0, keepdims=True)
        v_south = jnp.sum(hrows_ref[2] * from_rows[0, m], axis=0, keepdims=True)
        mass = sums_ref[m, 0] + jnp.where(lane == 0, at_west, 0.0) + jnp.where(lane == cols - 1, at_east, 0.0)
        mass = mass + jnp.where(row == 0, at_south, 0.0) - jnp.where(row == rows - 1, at_north, 0.0)
        total_s[m, 0] = mass
        total_s[m, 1] = sums_ref[m, 1] + jnp.where(lane == 0, u_west, 0.0)
        total_s[m, 2] = sums_ref[m, 2] + jnp.where(row == 0, v_south, 0.0)
    for d, out_ref in enumerate(outs):
        start = pl.multiple_of((mine ^ d) * height, height)
        out_ref[...] = total_s[:, :, pl.ds(start, height), :]


def stats_kernel(*refs):
    ins, out_ref = refs[:-1], refs[-1]
    members, fields = ins[0].shape[:2]
    count = len(ins) * members
    for f in range(fields):
        values = [ref[m, f] for ref in ins for m in range(members)]
        mean = functools.reduce(jnp.add, values) / count
        square = functools.reduce(jnp.add, [(v - mean) * (v - mean) for v in values]) / (count - 1)
        out_ref[f] = mean
        out_ref[fields + f] = square


def select_kernel(width, masks_ref, *refs):
    tiles, outs = refs[:-width], refs[-width:]
    for d, out_ref in enumerate(outs):
        for f in range(out_ref.shape[0]):
            value = tiles[0][f]
            for j in range(1, len(tiles)):
                value = jnp.where(masks_ref[j * width + d] > 0.5, tiles[j][f], value)
            out_ref[f] = value


def pick_kernel(masks_ref, *refs):
    ins, out_ref = refs[:-1], refs[-1]
    width = len(ins)
    base = masks_ref.shape[0] - width
    for f in range(ins[0].shape[0]):
        value = ins[0][f]
        for d in range(1, width):
            value = jnp.where(masks_ref[base + d] > 0.5, ins[d][f], value)
        out_ref[0, 0, f] = value


def call(kernel, outs, in_specs, scratch=(), limit=16):
    return pl.pallas_call(
        kernel,
        out_shape=[jax.ShapeDtypeStruct(s, jnp.float32) for s in outs],
        in_specs=in_specs,
        out_specs=[VMEM] * len(outs),
        scratch_shapes=list(scratch),
        compiler_params=pltpu.CompilerParams(vmem_limit_bytes=limit * 1024 * 1024),
    )


def permuted(block, axis, source):
    count = lax.axis_size(axis)
    return lax.ppermute(block, axis, [(source(i) % count, i) for i in range(count)])


def exchange(far, near, edge_rows):
    far = permuted(far, "tx", lambda i: i + 1 if i % 2 else i - 1)
    near = permuted(near, "tx", lambda i: i ^ 1)
    if lax.axis_size("ty") <= 2:
        both = permuted(edge_rows, "ty", lambda i: i - 1)
    else:
        south = permuted(edge_rows[0], "ty", lambda i: i - 1)
        north = permuted(edge_rows[1], "ty", lambda i: i + 1)
        both = jnp.stack([south, north])
    return far, near, both


def steps(pressure, east_wind, north_wind, vertical_wind, sound_squared, thickness, owner_map):
    members, levels, rows, cols = pressure.shape
    ranks, height_count, width = (lax.axis_size(a) for a in ("mem", "ty", "tx"))
    height = rows // ranks
    plane = (rows, cols)
    many = (members, levels, rows, cols)
    field = (levels, rows, cols)
    lines = (2, members, levels, cols)
    part = (6, height, cols)
    pressure, east_wind, north_wind, vertical_wind = (
        pltpu.with_memory_space_constraint(x, pltpu.HBM)
        for x in (pressure, east_wind, north_wind, vertical_wind)
    )
    far, near, edge_rows, p0, u0 = call(
        pack_kernel,
        [plane, plane, lines, many, many],
        [HBM] * 3,
        [
            pltpu.VMEM((members, levels, 8, cols), jnp.float32),
            pltpu.SemaphoreType.DMA((members, 3)),
        ],
        limit=PACK_LIMIT,
    )(pressure, east_wind, north_wind)
    far, near, both = exchange(far, near, edge_rows)
    hcols, hrows, hth, masks, e, inv, *weights, part0, u0, v0, w0 = call(
        prepare_kernel,
        [
            (rows, cols),
            (3, levels, cols),
            (8, cols),
            (height_count * width + width, 8, cols),
            *[field] * 9,
            *[many] * 3,
            vertical_wind.shape,
        ],
        [VMEM, VMEM, VMEM, HBM, HBM, SMEM, SMEM],
        [pltpu.SemaphoreType.DMA((2, members))],
        limit=PREP_LIMIT,
    )(sound_squared, p0, u0, north_wind, vertical_wind, thickness, owner_map)
    far, near, edge_rows, p1, zu, zv, w1 = call(
        solve_kernel, [plane, plane, lines, *[many] * 4], [VMEM] * 10
    )(sound_squared, part0, u0, v0, w0, e, inv, far, near, both)
    far, near, both = exchange(far, near, edge_rows)
    (sums,) = call(
        sum_kernel,
        [(members, 3, rows, cols)],
        [VMEM] * 4 + [SMEM] + [VMEM] * 7,
        [pltpu.VMEM((members, 3, rows, cols), jnp.float32)],
    )(p1, zu, zv, w1, thickness, *weights)
    quarters = call(
        edge_kernel,
        [(members, 3, height, cols)] * ranks,
        [VMEM] * 7,
        [pltpu.VMEM((members, 3, rows, cols), jnp.float32)],
    )(sums, far, near, both, hcols, hrows, hth)
    quarters = [
        permuted(x, "mem", lambda i, d=d: i ^ d) if d else x for d, x in enumerate(quarters)
    ]
    (stats,) = call(stats_kernel, [part], [VMEM] * ranks)(*quarters)
    tiles = [
        permuted(stats, "ty", lambda i, j=j: i ^ j) if j else stats
        for j in range(height_count)
    ]
    chosen = call(
        functools.partial(select_kernel, width), [part] * width, [VMEM] * (1 + height_count)
    )(masks, *tiles)
    routed = [permuted(x, "tx", lambda i, d=d: i ^ d) if d else x for d, x in enumerate(chosen)]
    (result,) = call(pick_kernel, [(1, 1) + part], [VMEM] * (1 + width))(masks, *routed)
    return result


def solution(mesh):
    placed = (
        P("mem", None, "ty", "tx"),
        P("mem", None, "ty", "tx"),
        P("mem", None, "ty", "tx"),
        P("mem", None, "ty", "tx"),
        P(None, "ty", "tx"),
        P(),
        P(),
    )
    return jax.shard_map(
        steps,
        mesh=mesh,
        in_specs=placed,
        out_specs=P("ty", "tx", None, "mem", None),
        check_vma=False,
    )
```
